32 devices in a mesh: dp: 16 (over z, y, core), level: 2 (over x).
Axes of the slice: x: 2, y: 2, z: 4, core: 2. Of those that a mesh axis runs over, the one named last changes fastest.
Arguments:
- token_ids: int32 [16, 2, 1536], P('dp', 'level'), may hold values from 0 to 1023
- decoded_mask: int32 [16, 2, 1536], P('dp', 'level'), may hold values 0 or 1
- levels_done: int32 [16], P('dp'), may hold values from 0 to 1
- code_tables: bfloat16 [2, 1024, 1024], P('level'), may hold values from -6 to 6
- mask_vectors: bfloat16 [2, 1024], P('level'), may hold values from -6 to 6
- w_qkv: bfloat16 [3, 1024, 1024], P(None, 'dp', 'level'), may hold values from -6 to 6
- w_out: bfloat16 [1024, 1024], P('level', 'dp'), may hold values from -0.1875 to 0.1875
- w_expand: bfloat16 [1024, 2048], P('dp'), may hold values from -0.1875 to 0.1875
- w_depth: bfloat16 [5, 1024], replicated, may hold values from -2.5 to 2.5
- w_project: bfloat16 [1024, 1024], P('dp'), may hold values from -0.1875 to 0.1875
- level_heads: bfloat16 [2, 1024, 1024], P('level'), may hold values from -0.1875 to 0.1875
Outputs:
- logits: bfloat16 [16, 2, 1536, 1024], P('dp', 'level')
The draws below stay inside these ranges and needn't reach their ends.
Inputs may be any that keep to these rules, and one draw needn't show every extreme that they name: `levels_done`: levels below it are fully decoded; the level equal to it is the one being decoded.
All inputs are finite; a program needn't handle non-finite values. No bound on the sum of `decoded_mask` on one device may be relied on, other than what follows from the above.
Results may differ from the reference program's by a relative error of at most 0.006.
Values may be sent and summed in bfloat16 or wider, within the bound.
A program may use at most 192 MiB of HBM per device.

```python
import jax
import jax.numpy as jnp
from jax import lax

D = 1024
HEADS = 16
VOCAB = 1024
FRAMES = 1536
KERNEL = 5
HEAD_DIM = 64
LEVELS = 2
CLIPS = 16


def draw_w_qkv(key, part):
    spread = D ** (-0.5)
    weights = jax.random.normal(jax.random.fold_in(key, 11), (3, D, D), jnp.float32) * spread
    weights = jnp.clip(weights, -6.0 * spread, 6.0 * spread)
    return jnp.clip(weights, -6.0, 6.0).astype(jnp.bfloat16)


def with_ends(values, key, low, top_value):
    longest = values.shape.index(max(values.shape))
    spots = []
    for shift in (0, 1):
        where = [jax.random.randint(jax.random.fold_in(key, axis), (), 0, length) for axis, length in enumerate(values.shape)]
        where[longest] = (where[longest] + shift) % values.shape[longest]
        spots.append(tuple(where))
    return values.at[spots[0]].set(low).at[spots[1]].set(top_value)


def block_scale(own_key, shape, split, low, top_value):
    gain = 1.0
    for dim, shards_of in split:
        steps = jax.random.uniform(jax.random.fold_in(jax.random.fold_in(own_key, 6), dim), (shards_of,), jnp.float32, low / len(split), top_value / len(split))
        gain = gain * jnp.repeat(jnp.exp(steps), shape[dim] // shards_of).reshape((-1,) + (1,) * (len(shape) - 1 - dim))
    return gain


def centred(stream_key, extent, width, bound, pieces=(), held_as=jnp.bfloat16):
    array = jax.random.normal(stream_key, extent, jnp.float32) * width
    if len(pieces) > 0:
        array = block_scale(stream_key, extent, pieces, -0.22, 0.18) * array
    return jnp.clip(array, min=-bound, max=bound).astype(held_as)


def setup_inputs(seed: int = 0) -> dict:
    streams_of = jax.random.split(jax.random.key(seed), 12)
    return {
        "token_ids": with_ends(jax.random.randint(streams_of[0], (CLIPS, LEVELS, FRAMES), 0, VOCAB), jax.random.fold_in(streams_of[0], 1), 0, VOCAB - 1).astype(jnp.int32),
        "decoded_mask": with_ends((jax.random.randint(streams_of[1], (CLIPS, LEVELS, FRAMES), 0, 2) < 1).astype(jnp.int32), jax.random.fold_in(streams_of[1], 1), 0, 1),
        "levels_done": with_ends(jax.random.randint(streams_of[2], (CLIPS,), 0, LEVELS), jax.random.fold_in(streams_of[2], 1), 0, LEVELS - 1).astype(jnp.int32),
        "code_tables": centred(streams_of[3], (LEVELS, VOCAB, D), 1.0, 6.0, ((0, 2),)),
        "mask_vectors": centred(streams_of[4], (LEVELS, D), 1.0, 6.0, ((0, 2),)),
        "w_qkv": draw_w_qkv(jax.random.fold_in(streams_of[11], 71), 0),
        "w_out": centred(streams_of[6], (D, D), D ** -0.5, 0.1875, ((0, 2), (1, 16))),
        "w_expand": centred(streams_of[7], (D, 2 * D), D ** -0.5, 0.1875, ((0, 16),)),
        "w_depth": centred(streams_of[8], (KERNEL, D), KERNEL ** -0.5, 2.5),
        "w_project": centred(streams_of[9], (D, D), D ** -0.5, 0.1875, ((0, 16),)),
        "level_heads": centred(streams_of[10], (LEVELS, D, VOCAB), D ** -0.5, 0.1875, ((0, 2),)),
    }


def layer_norm(values):
    centered = values - lax.optimization_barrier(jnp.mean(values, axis=-1, keepdims=True))
    variance = lax.optimization_barrier(jnp.mean(centered * centered, axis=-1, keepdims=True))
    return centered * lax.rsqrt(variance + 1e-05)

def clip_step(token_ids, decoded_mask, levels_done, code_tables, mask_vectors, w_qkv, w_out, w_expand, w_depth, w_project, level_heads):
    level_ids = jnp.arange(LEVELS, dtype=jnp.int32)[:, None]
    use_token = (level_ids < levels_done) | (level_ids == levels_done) & (decoded_mask == 1)
    picked = jax.vmap(lambda table_one, ids_one: jnp.take(table_one, ids_one, axis=0))(code_tables, token_ids.astype(jnp.int32)).astype(jnp.float32)
    terms = jnp.where(use_token[:, :, None], picked, mask_vectors.astype(jnp.float32)[:, None, :])
    embedded = lax.optimization_barrier(jnp.sum(terms, axis=0))
    normed = layer_norm(embedded).astype(jnp.bfloat16)
    queries = jnp.dot(normed, w_qkv[0], preferred_element_type=jnp.float32).astype(jnp.bfloat16)
    key_rows = jnp.dot(normed, w_qkv[1], preferred_element_type=jnp.float32).astype(jnp.bfloat16)
    value_rows = jnp.dot(normed, w_qkv[2], preferred_element_type=jnp.float32).astype(jnp.bfloat16)
    queries, key_rows, value_rows = lax.optimization_barrier((queries, key_rows, value_rows))
    query_three = queries.astype(jnp.float32).reshape(FRAMES, HEADS, HEAD_DIM)
    key_three = key_rows.astype(jnp.float32).reshape(FRAMES, HEADS, HEAD_DIM)
    value_three = value_rows.astype(jnp.float32).reshape(FRAMES, HEADS, HEAD_DIM)
    scores = jnp.einsum('qhd,khd->hqk', query_three, key_three) * HEAD_DIM ** (-0.5)
    row_max = lax.optimization_barrier(jnp.max(scores, axis=-1, keepdims=True))
    weights = jnp.exp(scores - row_max)
    weight_sum = lax.optimization_barrier(jnp.sum(weights, axis=-1))
    rounded = lax.optimization_barrier(weights.astype(jnp.bfloat16)).astype(jnp.float32)
    mixture = jnp.einsum('hqk,khd->qhd', rounded, value_three) / weight_sum.T[:, :, None]
    attended = mixture.reshape(FRAMES, D).astype(jnp.bfloat16)
    after_attn = embedded + jnp.dot(attended, w_out, preferred_element_type=jnp.float32)
    normed_two = layer_norm(after_attn).astype(jnp.bfloat16)
    gate_linear = jnp.dot(normed_two, w_expand, preferred_element_type=jnp.float32)
    gated = (gate_linear[:, :D] * jax.nn.sigmoid(gate_linear[:, D:])).astype(jnp.bfloat16)
    gated = lax.optimization_barrier(gated)
    half_width = KERNEL // 2
    padded = jnp.pad(gated.astype(jnp.float32), ((half_width, half_width), (0, 0)))
    conv = jnp.zeros((FRAMES, D), jnp.float32)
    for tap_index in range(KERNEL):
        conv = conv + padded[tap_index:tap_index + FRAMES] * w_depth[tap_index].astype(jnp.float32)
    activated = (conv * jax.nn.sigmoid(conv)).astype(jnp.bfloat16)
    after_conv = after_attn + jnp.dot(activated, w_project, preferred_element_type=jnp.float32)
    final_norm = layer_norm(after_conv).astype(jnp.bfloat16)
    return jax.vmap(lambda head_one: jnp.dot(final_norm, head_one, preferred_element_type=jnp.float32))(level_heads).astype(jnp.bfloat16)

def reference(token_ids, decoded_mask, levels_done, code_tables, mask_vectors, w_qkv, w_out, w_expand, w_depth, w_project, level_heads):

    def one_clip(clip_parts):
        return clip_step(clip_parts[0], clip_parts[1], clip_parts[2], code_tables, mask_vectors, w_qkv, w_out, w_expand, w_depth, w_project, level_heads)
    return lax.map(one_clip, (token_ids, decoded_mask, levels_done))
```

```python
import functools

import jax
import jax.numpy as jnp
from jax import lax
from jax.experimental import pallas as pl
from jax.experimental.pallas import tpu as pltpu
from jax.sharding import PartitionSpec as P

HEADS = 16
CORES = 2
LANES = 128
PAD = 16
MESH = pl.DeviceIdType.MESH


def layer_norm(values):
    centered = values - jnp.mean(values, axis=-1, keepdims=True)
    variance = jnp.mean(centered * centered, axis=-1, keepdims=True)
    return centered * lax.rsqrt(variance + 1e-05)


def dot_f32(left, right):
    return jnp.dot(left, right, preferred_element_type=jnp.float32)


def dot_nt(left, right):
    return lax.dot_general(left, right, (((1,), (1,)), ((), ())), preferred_element_type=jnp.float32)


def chip_at(position, chips):
    position = lax.rem(position + 2 * chips, chips)
    turned = position // (chips // 2)
    return (1 - turned) * 2 * position + turned * (2 * (chips - 1 - position) + 1)


def position_of(chip, chips):
    odd = lax.rem(chip, 2)
    return (1 - odd) * (chip // 2) + odd * (chips - 1 - chip // 2)


class Ring:
    def __init__(self, full, own, rows, chips, sems):
        self.full, self.own, self.rows, self.chips, self.half = full, own, rows, chips, chips // 2
        self.send, self.recv, self.sib_send, self.sib_recv = sems
        self.device = lax.axis_index("dp")
        self.core = lax.rem(self.device, CORES)
        self.position = position_of(self.device // CORES, chips)

    def block(self, position, core, part):
        row = (chip_at(position, self.chips) * CORES + core) * self.rows
        count = self.rows
        if part is not None:
            count = self.rows // 2
            row = row + part * count
        return self.full.at[pl.ds(pl.multiple_of(row, count), count), :]

    def own_block(self, part):
        if self.own is None:
            return self.block(self.position, self.core, part)
        if part is None:
            return self.own
        count = self.rows // 2
        return self.own.at[pl.ds(part * count, count), :]

    def part(self, way, step):
        return way if step == self.half - 1 else None

    def origin(self, way, step):
        return self.position - (1 + step) if way == 0 else self.position + (1 + step)

    def hop(self, way, step):
        towards = self.position + 1 if way == 0 else self.position - 1
        source = self.position - step if way == 0 else self.position + step
        part = self.part(way, step)
        place = self.block(source, self.core, part)
        target = chip_at(towards, self.chips) * CORES + self.core
        return pltpu.make_async_remote_copy(
            src_ref=self.own_block(part) if step == 0 else place,
            dst_ref=place,
            send_sem=self.send.at[way, step],
            recv_sem=self.recv.at[way, step],
            device_id={"dp": target},
            device_id_type=MESH,
        )

    def arrival(self, way, step):
        ref = self.block(self.origin(way, step), self.core, self.part(way, step))
        return pltpu.make_async_remote_copy(
            src_ref=ref,
            dst_ref=ref,
            send_sem=self.send.at[way, step],
            recv_sem=self.recv.at[way, step],
            device_id={"dp": self.device},
            device_id_type=MESH,
        )

    def share(self, way, step, core):
        position = self.position if step < 0 else self.origin(way, step)
        place = self.block(position, core, None if step < 0 else self.part(way, step))
        sibling = self.device + 1 - 2 * self.core
        return pltpu.make_async_remote_copy(
            src_ref=self.own_block(None) if step < 0 else place,
            dst_ref=place,
            send_sem=self.sib_send.at[way, step + 1],
            recv_sem=self.sib_recv.at[way, step + 1],
            device_id={"dp": sibling},
            device_id_type=MESH,
        )

    def start(self):
        for way in range(2):
            self.hop(way, 0).start()
        self.share(0, -1, self.core).start()

    def advance(self, step):
        for way in range(2):
            self.arrival(way, step).wait_recv()
            if step + 1 < self.half:
                self.hop(way, step + 1).start()
            self.share(way, step, self.core).start()

    def finish(self):
        for way in range(2):
            for step in range(self.half):
                self.hop(way, step).wait_send()
                self.share(way, step, self.core).wait_send()
                self.share(way, step, 1 - self.core).wait_recv()
        self.share(0, -1, self.core).wait_send()
        self.share(0, -1, 1 - self.core).wait_recv()


def step_kernel(
    levels, devices, frames, width,
    tok_ref, dec_ref, done_ref, fill_ref, table_ref, qkv_ref, out_ref, expand_ref, project_ref, depth_ref,
    final_ref,
    toks, decs, fills, ids, tables, proj, rest, embedded, keys, values_t, queries,
    attended, gated, final, scores_a, scores_b, peaks_a, peaks_b,
    local_sem, level_send, level_recv, table_send, table_recv, att_send, att_recv, final_sem,
    ring_a, ring_a_recv, sib_a, sib_a_recv, ring_b, ring_b_recv, sib_b, sib_b_recv,
):
    level = lax.axis_index("level")
    device = lax.axis_index("dp")
    core = lax.rem(device, CORES)
    sibling = device + 1 - 2 * core
    chips = devices // CORES
    rows = width // devices
    columns = width // levels
    codes = table_ref.shape[0]
    position = position_of(device // CORES, chips)
    bf16 = jnp.bfloat16

    barrier = pltpu.get_barrier_semaphore()
    for shift in range(1, levels):
        pl.semaphore_signal(barrier, inc=1, device_id={"level": lax.rem(level + shift, levels)}, device_id_type=MESH)
    for other in (
        sibling,
        chip_at(position + 1, chips) * CORES + core,
        chip_at(position - 1, chips) * CORES + core,
    ):
        pl.semaphore_signal(barrier, inc=1, device_id={"dp": other}, device_id_type=MESH)

    own_rows = pl.ds(pl.multiple_of(device * rows, rows), rows)
    own_columns = pl.ds(pl.multiple_of(level * columns, columns), columns)
    sources = (tok_ref, dec_ref, fill_ref, out_ref)

    def place_of(kind, owner):
        owner_columns = pl.ds(pl.multiple_of(owner * columns, columns), columns)
        return (toks.at[owner], decs.at[owner], fills.at[owner], rest.at[0, own_rows, owner_columns])[kind]

    def over_level(kind, shift):
        return pltpu.make_async_remote_copy(
            src_ref=sources[kind], dst_ref=place_of(kind, level),
            send_sem=level_send.at[kind, shift], recv_sem=level_recv.at[kind, shift],
            device_id={"level": lax.rem(level + shift, levels)}, device_id_type=MESH,
        )

    def from_level(kind, shift):
        sender = lax.rem(level + levels - shift, levels)
        return pltpu.make_async_remote_copy(
            src_ref=sources[kind], dst_ref=place_of(kind, sender),
            send_sem=level_send.at[kind, shift], recv_sem=level_recv.at[kind, shift],
            device_id={"level": sender}, device_id_type=MESH,
        )

    piece = LANES
    chunk = CORES * piece
    chunks = codes // chunk

    def chunk_rows(order, which):
        return pl.ds(pl.multiple_of((order * CORES + which) * piece, piece), piece)

    def table_out(order, shift):
        return pltpu.make_async_remote_copy(
            src_ref=table_ref.at[chunk_rows(order, core)], dst_ref=tables.at[level, chunk_rows(order, core)],
            send_sem=table_send.at[0, shift, order], recv_sem=table_recv.at[0, shift, order],
            device_id={"level": lax.rem(level + shift, levels)}, device_id_type=MESH,
        )

    def table_at(order, shift, which, kind):
        place = tables.at[lax.rem(level + levels - shift, levels), chunk_rows(order, which)]
        return pltpu.make_async_remote_copy(
            src_ref=place, dst_ref=place,
            send_sem=table_send.at[kind, shift, order], recv_sem=table_recv.at[kind, shift, order],
            device_id={"dp": sibling}, device_id_type=MESH,
        )

    early = [
        pltpu.make_async_copy(sources[kind], place_of(kind, level), local_sem.at[kind]) for kind in range(3)
    ] + [pltpu.make_async_copy(table_ref, tables.at[level], local_sem.at[3])]
    late = [
        pltpu.make_async_copy(qkv_ref.at[part], proj.at[part, own_rows, :], local_sem.at[4 + part]) for part in range(3)
    ] + [
        pltpu.make_async_copy(out_ref, place_of(3, level), local_sem.at[7]),
        pltpu.make_async_copy(expand_ref.at[:, pl.ds(0, width)], rest.at[1, own_rows, :], local_sem.at[8]),
        pltpu.make_async_copy(expand_ref.at[:, pl.ds(width, width)], rest.at[2, own_rows, :], local_sem.at[9]),
        pltpu.make_async_copy(project_ref, rest.at[3, own_rows, :], local_sem.at[10]),
    ]
    for copy in early + late:
        copy.start()

    def rings(full, own, count, sems):
        return [
            Ring(full.at[part], own(part), rows, chips, tuple(sem.at[part] for sem in sems))
            for part in range(count)
        ]

    first = rings(proj, lambda part: qkv_ref.at[part], 3, (ring_a, ring_a_recv, sib_a, sib_a_recv))
    second = rings(rest, lambda part: None, 4, (ring_b, ring_b_recv, sib_b, sib_b_recv))
    hops = chips // 2

    pl.semaphore_wait(barrier, levels + 2)
    for kind in range(3):
        for shift in range(1, levels):
            over_level(kind, shift).start()
    for ring in first:
        ring.start()
    for order in range(chunks):
        for shift in range(1, levels):
            table_out(order, shift).start()
        if order == 0:
            for shift in range(1, levels):
                over_level(3, shift).start()

    for pair in range(values_t.shape[0]):
        values_t[pair, LANES:, :] = jnp.ones((values_t.shape[1] - LANES, frames), bf16)
    for place in (pl.ds(0, PAD), pl.ds(PAD + frames, PAD)):
        gated[place, :] = jnp.zeros((PAD, width), bf16)

    for copy in early:
        copy.wait()
    for kind in range(3):
        for shift in range(1, levels):
            from_level(kind, shift).wait_recv()

    done = done_ref[0]
    for row in range(levels):
        use = (row < done) | ((row == done) & (decs[row] == 1))
        code = jnp.where(use, toks[row], -1).astype(jnp.float32)
        for base in range(0, frames, LANES):
            ids[row, base : base + LANES, :] = jnp.broadcast_to(code[:, base : base + LANES], (LANES, LANES)).T

    tile = 2 * LANES
    tiles = frames // tile
    lane = lax.broadcasted_iota(jnp.int32, (tile, LANES), 1).astype(jnp.float32)

    def span_of(step):
        return pl.ds(pl.multiple_of(step * tile, tile), tile)

    def onehot(found, start, count):
        return jnp.concatenate(
            [jnp.where(found - start == lane + float(base), 1.0, 0.0).astype(bf16) for base in range(0, count, LANES)],
            axis=1,
        )

    @pl.loop(0, tiles)
    def _(step):
        @pl.when(step == tiles // 2)
        def _():
            for ring in first:
                ring.advance(0)

        span = span_of(step)
        total = dot_f32(onehot(ids[level, span, :], 0.0, codes), tables[level])
        for row in range(levels):
            total = total + jnp.where(ids[row, span, 0:1] < 0.0, fills[row].astype(jnp.float32), 0.0)
        embedded[span, :] = total

    @pl.loop(0, chunks)
    def _(order):
        begin = (order * chunk).astype(jnp.float32)
        codes_at = pl.ds(pl.multiple_of(order * chunk, chunk), chunk)
        for shift in range(1, levels):
            sender = lax.rem(level + levels - shift, levels)
            table_at(order, shift, core, 0).wait_recv()
            table_at(order, shift, core, 1).start()
            table_at(order, shift, 1 - core, 1).wait_recv()

            @pl.loop(0, tiles)
            def _(step):
                span = span_of(step)
                found = onehot(ids[sender, span, :], begin, chunk)
                embedded[span, :] = embedded[span, :] + dot_f32(found, tables[sender, codes_at, :])

        for step in range(1, hops):
            @pl.when(order == (step - 1) * chunks // (hops - 1))
            def _():
                for ring in first:
                    ring.advance(step)
                if step == max(hops - 2, 1):
                    for copy in late:
                        copy.wait()
                    for shift in range(1, levels):
                        from_level(3, shift).wait_recv()
                    for ring in second:
                        ring.start()

    for ring in first:
        ring.finish()

    head_dim = width // HEADS
    scale = head_dim ** (-0.5)
    pairs = columns // LANES

    @pl.loop(0, tiles)
    def _(step):
        for part, ring in enumerate(second):
            @pl.when(step == min(max(2 * part - 2, 0), tiles - 1))
            def _():
                ring.advance(0)

        span = span_of(step)
        normed = layer_norm(embedded[span, :]).astype(bf16)
        queries[span, :] = dot_f32(normed, proj[0]).astype(bf16) * jnp.asarray(scale, bf16)
        keys[span, :] = dot_f32(normed, proj[1]).astype(bf16)
        found = dot_f32(normed, proj[2])
        for pair in range(pairs):
            values_t[pair, 0:LANES, span] = found[:, pair * LANES : (pair + 1) * LANES].T.astype(bf16)

    block = LANES
    stages = frames // block

    def rows_of(stage):
        return pl.ds(pl.multiple_of(stage * block, block), block)

    def attended_copy(stage, shift, owner, target):
        owner_columns = pl.ds(pl.multiple_of(owner * columns, columns), columns)
        place = attended.at[rows_of(stage), owner_columns]
        return pltpu.make_async_remote_copy(
            src_ref=place, dst_ref=place,
            send_sem=att_send.at[stage, shift], recv_sem=att_recv.at[stage, shift],
            device_id={"level": target}, device_id_type=MESH,
        )

    def attended_out(stage, shift):
        return attended_copy(stage, shift, level, lax.rem(level + shift, levels))

    def attended_in(stage, shift):
        sender = lax.rem(level + levels - shift, levels)
        return attended_copy(stage, shift, sender, sender)

    lower = lax.broadcasted_iota(jnp.int32, (block, LANES), 1) < head_dim
    buffers = ((scores_a, peaks_a), (scores_b, peaks_b))

    def score_pair(stage, pair, buffer):
        store, peaks = buffer
        across = pl.ds(pair * LANES, LANES)
        query = queries[rows_of(stage), across]
        zero = jnp.zeros_like(query)
        both = jnp.concatenate([jnp.where(lower, query, zero), jnp.where(lower, zero, query)], axis=0)
        found = dot_nt(keys[:, across], both)
        store[...] = found
        peaks[...] = jnp.max(found.reshape(frames // 8, 8, CORES * block), axis=0)

    def mix_pair(stage, pair, buffer):
        store, peaks = buffer
        peak = jnp.max(peaks[...], axis=0, keepdims=True)
        weights = jnp.exp(store[...] - peak).astype(bf16)
        mixed = dot_f32(values_t[pair], weights)
        inverse = 1.0 / mixed[LANES : LANES + 1, :]
        low = mixed[0:head_dim, 0:block] * inverse[:, 0:block]
        high = mixed[head_dim : 2 * head_dim, block:] * inverse[:, block:]
        across = pl.ds(pl.multiple_of(level * columns + pair * LANES, LANES), LANES)
        attended[rows_of(stage), across] = jnp.concatenate([low, high], axis=0).T.astype(bf16)

    per_turn = 1 if pairs % 2 == 0 else 2
    units = [(ahead, pair) for ahead in range(per_turn) for pair in range(pairs)]
    events = [(step, ring) for step in range(1, hops) for ring in second]
    turns = stages // per_turn

    score_pair(0, 0, buffers[0])

    @pl.loop(0, turns)
    def _(turn):
        for event, (step, ring) in enumerate(events):
            @pl.when(turn == event * turns // len(events))
            def _():
                ring.advance(step)

        @pl.when(turn > 0)
        def _():
            for ahead in range(per_turn):
                for shift in range(1, levels):
                    attended_out((turn - 1) * per_turn + ahead, shift).start()

        for index, (ahead, pair) in enumerate(units):
            if index + 1 < len(units):
                next_ahead, next_pair = units[index + 1]
                next_stage = turn * per_turn + next_ahead
            else:
                next_pair = 0
                next_stage = lax.min((turn + 1) * per_turn, stages - 1)
            score_pair(next_stage, next_pair, buffers[(index + 1) % 2])
            mix_pair(turn * per_turn + ahead, pair, buffers[index % 2])

    for ahead in range(per_turn):
        for shift in range(1, levels):
            attended_out((turns - 1) * per_turn + ahead, shift).start()
    for ring in second:
        ring.finish()

    taps = depth_ref.shape[0]
    depth = depth_ref[...].astype(jnp.float32)

    def gate(step):
        for ahead in range(tile // block):
            for shift in range(1, levels):
                attended_in(step * (tile // block) + ahead, shift).wait_recv()
        span = span_of(step)
        after_attn = embedded[span, :] + dot_nt(attended[span, :], rest[0])
        embedded[span, :] = after_attn
        normed = layer_norm(after_attn).astype(bf16)
        mixed = dot_f32(normed, rest[1]) * jax.nn.sigmoid(dot_f32(normed, rest[2]))
        gated[pl.ds(pl.multiple_of(PAD + step * tile, PAD), tile), :] = mixed.astype(bf16)

    def final_copy(step):
        span = span_of(step)
        return pltpu.make_async_copy(final.at[span], final_ref.at[span], final_sem.at[step])

    def convolve(step):
        span = span_of(step)
        start = pl.multiple_of(step * tile, tile)
        window = gated[pl.ds(start, tile + 2 * PAD), :].astype(jnp.float32)
        conv = jnp.zeros((tile, width), jnp.float32)
        for tap in range(taps):
            first_row = PAD - taps // 2 + tap
            conv = conv + window[first_row : first_row + tile] * depth[tap : tap + 1, :]
        activated = (conv * jax.nn.sigmoid(conv)).astype(bf16)
        after_conv = embedded[span, :] + dot_f32(activated, rest[3])
        final[span, :] = layer_norm(after_conv).astype(bf16)
        final_copy(step).start()

    gate(0)

    @pl.loop(0, tiles - 1)
    def _(step):
        gate(step + 1)
        convolve(step)

    convolve(tiles - 1)

    for shift in range(1, levels):
        for kind in range(4):
            over_level(kind, shift).wait_send()

        @pl.loop(0, chunks)
        def _(order):
            table_out(order, shift).wait_send()
            table_at(order, shift, core, 1).wait_send()

        @pl.loop(0, stages)
        def _(stage):
            attended_out(stage, shift).wait_send()

    @pl.loop(0, tiles)
    def _(step):
        final_copy(step).wait()


def decode_step(levels, devices, tokens, decoded, done, fill, table, w_qkv, w_out_t, w_expand, w_project, taps):
    frames, width = tokens.shape[1], table.shape[1]
    chips = devices // CORES
    columns = width // levels
    chunks = table.shape[0] // (CORES * LANES)
    stages = frames // LANES
    tiles = frames // (2 * LANES)
    vmem = pl.BlockSpec(memory_space=pltpu.VMEM)
    anywhere = pl.BlockSpec(memory_space=pl.ANY)
    dma = pltpu.SemaphoreType.DMA
    half = chips // 2
    bf16, f32 = jnp.bfloat16, jnp.float32
    return pl.pallas_call(
        functools.partial(step_kernel, levels, devices, frames, width),
        out_shape=jax.ShapeDtypeStruct((frames, width), bf16),
        in_specs=[anywhere] * 2 + [pl.BlockSpec(memory_space=pltpu.SMEM)] + [anywhere] * 6 + [vmem],
        out_specs=anywhere,
        scratch_shapes=[
            pltpu.VMEM((levels,) + tokens.shape, jnp.int32),
            pltpu.VMEM((levels,) + decoded.shape, jnp.int32),
            pltpu.VMEM((levels,) + fill.shape, bf16),
            pltpu.VMEM((levels, frames, LANES), f32),
            pltpu.VMEM((levels,) + table.shape, bf16),
            pltpu.VMEM((3, width, columns), bf16),
            pltpu.VMEM((4, width, width), bf16),
            pltpu.VMEM((frames, width), f32),
            pltpu.VMEM((frames, columns), bf16),
            pltpu.VMEM((columns // LANES, LANES + 16, frames), bf16),
            pltpu.VMEM((frames, columns), bf16),
            pltpu.VMEM((frames, width), bf16),
            pltpu.VMEM((frames + 2 * PAD, width), bf16),
            pltpu.VMEM((frames, width), bf16),
            pltpu.VMEM((frames, 2 * LANES), f32),
            pltpu.VMEM((frames, 2 * LANES), f32),
            pltpu.VMEM((8, 2 * LANES), f32),
            pltpu.VMEM((8, 2 * LANES), f32),
            dma((11,)),
            dma((4, levels)), dma((4, levels)), dma((2, levels, chunks)), dma((2, levels, chunks)),
            dma((stages, levels)), dma((stages, levels)), dma((tiles,)),
        ]
        + [
            dma((count, 2, half + extra)) for count in (3, 4) for extra in (0, 0, 1, 1)
        ],
        compiler_params=pltpu.CompilerParams(
            collective_id=0, has_side_effects=True, vmem_limit_bytes=64000 * 1024
        ),
    )(tokens, decoded, done, fill, table, w_qkv, w_out_t, w_expand, w_project, taps)


def body(
    token_ids,
    decoded_mask,
    levels_done,
    code_tables,
    mask_vectors,
    w_qkv,
    w_out,
    w_expand,
    w_depth,
    w_project,
    level_heads,
):
    final = decode_step(
        lax.axis_size("level"), lax.axis_size("dp"), token_ids[0], decoded_mask[0], levels_done, mask_vectors,
        code_tables[0], w_qkv, w_out.T, w_expand, w_project, w_depth,
    )
    return dot_f32(final, level_heads[0]).astype(jnp.bfloat16)[None, None]


def solution(mesh):
    return jax.shard_map(
        body,
        mesh=mesh,
        in_specs=(
            P("dp", "level", None),
            P("dp", "level", None),
            P("dp"),
            P("level", None, None),
            P("level", None),
            P(None, "dp", "level"),
            P("level", "dp"),
            P("dp", None),
            P(),
            P("dp", None),
            P("level", None, None),
        ),
        out_specs=P("dp", "level", None, None),
        check_vma=False,
    )
```

```python
import functools

import jax
import jax.numpy as jnp
from jax import lax
from jax.experimental import pallas as pl
from jax.experimental.pallas import tpu as pltpu
from jax.sharding import PartitionSpec as P

HEADS = 16
CORES = 2
LANES = 128
PAD = 16
MESH = pl.DeviceIdType.MESH


def layer_norm(values):
    centered = values - jnp.mean(values, axis=-1, keepdims=True)
    variance = jnp.mean(centered * centered, axis=-1, keepdims=True)
    return centered * lax.rsqrt(variance + 1e-05)


def dot_f32(left, right):
    return jnp.dot(left, right, preferred_element_type=jnp.float32)


def dot_nt(left, right):
    return lax.dot_general(left, right, (((1,), (1,)), ((), ())), preferred_element_type=jnp.float32)


def chip_at(position, chips):
    position = lax.rem(position + 2 * chips, chips)
    turned = position // (chips // 2)
    return (1 - turned) * 2 * position + turned * (2 * (chips - 1 - position) + 1)


def position_of(chip, chips):
    odd = lax.rem(chip, 2)
    return (1 - odd) * (chip // 2) + odd * (chips - 1 - chip // 2)


class Ring:
    def __init__(self, full, own, rows, chips, sems):
        self.full, self.own, self.rows, self.chips, self.half = full, own, rows, chips, chips // 2
        self.send, self.recv, self.sib_send, self.sib_recv = sems
        self.device = lax.axis_index("dp")
        self.core = lax.rem(self.device, CORES)
        self.position = position_of(self.device // CORES, chips)

    def block(self, position, core, part):
        row = (chip_at(position, self.chips) * CORES + core) * self.rows
        count = self.rows
        if part is not None:
            count = self.rows // 2
            row = row + part * count
        return self.full.at[pl.ds(pl.multiple_of(row, count), count), :]

    def own_block(self, part):
        if self.own is None:
            return self.block(self.position, self.core, part)
        if part is None:
            return self.own
        count = self.rows // 2
        return self.own.at[pl.ds(part * count, count), :]

    def part(self, way, step):
        return way if step == self.half - 1 else None

    def origin(self, way, step):
        return self.position - (1 + step) if way == 0 else self.position + (1 + step)

    def hop(self, way, step):
        towards = self.position + 1 if way == 0 else self.position - 1
        source = self.position - step if way == 0 else self.position + step
        part = self.part(way, step)
        place = self.block(source, self.core, part)
        target = chip_at(towards, self.chips) * CORES + self.core
        return pltpu.make_async_remote_copy(
            src_ref=self.own_block(part) if step == 0 else place,
            dst_ref=place,
            send_sem=self.send,
            recv_sem=self.recv.at[way, step],
            device_id={"dp": target},
            device_id_type=MESH,
        )

    def arrival(self, way, step):
        ref = self.block(self.origin(way, step), self.core, self.part(way, step))
        return pltpu.make_async_remote_copy(
            src_ref=ref,
            dst_ref=ref,
            send_sem=self.send,
            recv_sem=self.recv.at[way, step],
            device_id={"dp": self.device},
            device_id_type=MESH,
        )

    def share(self, way, step, core):
        position = self.position if step < 0 else self.origin(way, step)
        place = self.block(position, core, None if step < 0 else self.part(way, step))
        sibling = self.device + 1 - 2 * self.core
        return pltpu.make_async_remote_copy(
            src_ref=self.own_block(None) if step < 0 else place,
            dst_ref=place,
            send_sem=self.sib_send,
            recv_sem=self.sib_recv,
            device_id={"dp": sibling},
            device_id_type=MESH,
        )

    def start(self):
        for way in range(2):
            self.hop(way, 0).start()
        self.share(0, -1, self.core).start()

    def advance(self, step):
        for way in range(2):
            self.arrival(way, step).wait_recv()
            if step + 1 < self.half:
                self.hop(way, step + 1).start()
            self.share(way, step, self.core).start()

    def all_of(self, blocks, send, recv):
        ref = self.full.at[pl.ds(0, blocks * self.rows), :]
        return pltpu.make_async_remote_copy(
            src_ref=ref,
            dst_ref=ref,
            send_sem=send,
            recv_sem=recv,
            device_id={"dp": self.device},
            device_id_type=MESH,
        )

    def finish(self):
        self.all_of(self.chips - 1, self.send, self.sib_recv).wait_send()
        shared = self.all_of(self.chips, self.sib_send, self.sib_recv)
        shared.wait_send()
        shared.wait_recv()


def step_kernel(
    levels, devices, frames, width,
    tok_ref, dec_ref, done_ref, fill_ref, table_ref, qkv_ref, out_ref, expand_ref, project_ref, depth_ref,
    final_ref,
    toks, decs, fills, ids, tables, proj, rest, embedded, keys, values_t, queries,
    normed_a, normed_b, attended, gated, final, scores_a, scores_b, peaks_a, peaks_b,
    local_sem, level_send, level_recv, table_send, table_recv, att_send, att_recv, final_sem,
    ring_a, ring_a_recv, sib_a, sib_a_recv, ring_b, ring_b_recv, sib_b, sib_b_recv,
):
    level = lax.axis_index("level")
    device = lax.axis_index("dp")
    core = lax.rem(device, CORES)
    sibling = device + 1 - 2 * core
    chips = devices // CORES
    rows = width // devices
    columns = width // levels
    codes = table_ref.shape[0]
    position = position_of(device // CORES, chips)
    bf16 = jnp.bfloat16

    barrier = pltpu.get_barrier_semaphore()
    for shift in range(1, levels):
        pl.semaphore_signal(barrier, inc=1, device_id={"level": lax.rem(level + shift, levels)}, device_id_type=MESH)
    for other in (
        sibling,
        chip_at(position + 1, chips) * CORES + core,
        chip_at(position - 1, chips) * CORES + core,
    ):
        pl.semaphore_signal(barrier, inc=1, device_id={"dp": other}, device_id_type=MESH)

    own_rows = pl.ds(pl.multiple_of(device * rows, rows), rows)
    own_columns = pl.ds(pl.multiple_of(level * columns, columns), columns)
    sources = (tok_ref, dec_ref, fill_ref, out_ref)

    def place_of(kind, owner):
        owner_columns = pl.ds(pl.multiple_of(owner * columns, columns), columns)
        return (toks.at[owner], decs.at[owner], fills.at[owner], rest.at[0, own_rows, owner_columns])[kind]

    def over_level(kind, shift):
        return pltpu.make_async_remote_copy(
            src_ref=sources[kind], dst_ref=place_of(kind, level),
            send_sem=level_send.at[kind, shift], recv_sem=level_recv.at[kind, shift],
            device_id={"level": lax.rem(level + shift, levels)}, device_id_type=MESH,
        )

    def from_level(kind, shift):
        sender = lax.rem(level + levels - shift, levels)
        return pltpu.make_async_remote_copy(
            src_ref=sources[kind], dst_ref=place_of(kind, sender),
            send_sem=level_send.at[kind, shift], recv_sem=level_recv.at[kind, shift],
            device_id={"level": sender}, device_id_type=MESH,
        )

    piece = LANES
    chunk = CORES * piece
    chunks = codes // chunk

    def chunk_rows(order, which):
        return pl.ds(pl.multiple_of((order * CORES + which) * piece, piece), piece)

    def table_out(order, shift):
        return pltpu.make_async_remote_copy(
            src_ref=table_ref.at[chunk_rows(order, core)], dst_ref=tables.at[level, chunk_rows(order, core)],
            send_sem=table_send.at[0, shift], recv_sem=table_recv.at[0, shift, order],
            device_id={"level": lax.rem(level + shift, levels)}, device_id_type=MESH,
        )

    def table_at(order, shift, which, kind):
        place = tables.at[lax.rem(level + levels - shift, levels), chunk_rows(order, which)]
        return pltpu.make_async_remote_copy(
            src_ref=place, dst_ref=place,
            send_sem=table_send.at[kind, shift], recv_sem=table_recv.at[kind, shift, order],
            device_id={"dp": sibling}, device_id_type=MESH,
        )

    early = [
        pltpu.make_async_copy(sources[kind], place_of(kind, level), local_sem.at[kind]) for kind in range(3)
    ] + [pltpu.make_async_copy(table_ref, tables.at[level], local_sem.at[3])]
    late = [
        pltpu.make_async_copy(qkv_ref.at[part], proj.at[part, own_rows, :], local_sem.at[4 + part]) for part in range(3)
    ] + [
        pltpu.make_async_copy(out_ref, place_of(3, level), local_sem.at[7]),
        pltpu.make_async_copy(expand_ref.at[:, pl.ds(0, width)], rest.at[1, own_rows, :], local_sem.at[8]),
        pltpu.make_async_copy(expand_ref.at[:, pl.ds(width, width)], rest.at[2, own_rows, :], local_sem.at[9]),
        pltpu.make_async_copy(project_ref, rest.at[3, own_rows, :], local_sem.at[10]),
    ]
    for copy in early + late:
        copy.start()

    def rings(full, own, count, sems):
        return [
            Ring(full.at[part], own(part), rows, chips, tuple(sem.at[part] for sem in sems))
            for part in range(count)
        ]

    first = rings(proj, lambda part: qkv_ref.at[part], 3, (ring_a, ring_a_recv, sib_a, sib_a_recv))
    rest_sources = (
        None, expand_ref.at[:, pl.ds(0, width)], expand_ref.at[:, pl.ds(width, width)], project_ref,
    )
    second = rings(rest, lambda part: rest_sources[part], 4, (ring_b, ring_b_recv, sib_b, sib_b_recv))
    hops = chips // 2
    turn = (1, 2, 0, 3)
    slots = ("c1", "c2", "c3", "c3", "q0", "q1", "s0", "s1", "s2", "s2", "s3", "s4", "s4", "s5", "s5", "end")
    plan = {}

    def at_slot(slot, act):
        plan.setdefault(slot, []).append(act)

    def run(slot):
        for act in plan.get(slot, ()):
            act()

    def start_second(part):
        if part == 0:
            for copy in late:
                copy.wait()
            for shift in range(1, levels):
                from_level(3, shift).wait_recv()
        second[part].start()

    for step in range(hops):
        slot = ("e", "c0", "c1", "c2")[step * 4 // hops]
        for ring in first:
            at_slot(slot, functools.partial(ring.advance, step))
    for slot, part in zip(("start", "e", "c0", "c1"), turn):
        at_slot(slot, functools.partial(start_second, part))
    order_of = [(step, part) for step in range(hops) for part in turn]
    for index, (step, part) in enumerate(order_of):
        at_slot(slots[index * len(slots) // len(order_of)], functools.partial(second[part].advance, step))

    pl.semaphore_wait(barrier, levels + 2)
    for kind in range(3):
        for shift in range(1, levels):
            over_level(kind, shift).start()
    for ring in first:
        ring.start()
    run("start")
    for shift in range(1, levels):
        over_level(3, shift).start()
    for order in range(chunks):
        for shift in range(1, levels):
            table_out(order, shift).start()

    head_dim = width // HEADS
    heads = columns // head_dim
    for head in range(heads):
        values_t[head, head_dim:, :] = jnp.ones((values_t.shape[1] - head_dim, frames), bf16)
    for place in (pl.ds(0, PAD), pl.ds(PAD + frames, PAD)):
        gated[place, :] = jnp.zeros((PAD, width), bf16)

    for copy in early:
        copy.wait()
    for kind in range(3):
        for shift in range(1, levels):
            from_level(kind, shift).wait_recv()

    done = done_ref[0]
    for row in range(levels):
        use = (row < done) | ((row == done) & (decs[row] == 1))
        code = jnp.where(use, toks[row], -1).astype(jnp.float32)
        for base in range(0, frames, LANES):
            ids[row, base : base + LANES, :] = jnp.broadcast_to(code[:, base : base + LANES], (LANES, LANES)).T

    tile = 2 * LANES
    tiles = frames // tile
    lane = lax.broadcasted_iota(jnp.int32, (tile, LANES), 1).astype(jnp.float32)

    def span_of(step):
        return pl.ds(pl.multiple_of(step * tile, tile), tile)

    def onehot(found, start, count):
        return jnp.concatenate(
            [jnp.where(found - start == lane + float(base), 1.0, 0.0).astype(bf16) for base in range(0, count, LANES)],
            axis=1,
        )

    @pl.loop(0, tiles)
    def _(step):
        @pl.when(step == tiles // 2)
        def _():
            run("e")

        span = span_of(step)
        total = dot_f32(onehot(ids[level, span, :], 0.0, codes), tables[level])
        for row in range(levels):
            total = total + jnp.where(ids[row, span, 0:1] < 0.0, fills[row].astype(jnp.float32), 0.0)
        embedded[span, :] = total

    def receive(order, shift):
        table_at(order, shift, core, 0).wait_recv()
        table_at(order, shift, core, 1).start()
        table_at(order, shift, 1 - core, 1).wait_recv()

    def picked(order, shift, span):
        sender = lax.rem(level + levels - shift, levels)
        found = onehot(ids[sender, span, :], lax.convert_element_type(order * chunk, jnp.float32), chunk)
        return dot_f32(found, tables[sender, pl.ds(pl.multiple_of(order * chunk, chunk), chunk), :])

    def add_chunk(order, shift):
        receive(order, shift)

        @pl.loop(0, tiles)
        def _(step):
            span = span_of(step)
            embedded[span, :] = embedded[span, :] + picked(order, shift, span)

    @pl.loop(0, chunks - 1)
    def _(order):
        for shift in range(1, levels):
            add_chunk(order, shift)
        for quarter in range(3):
            @pl.when(order == quarter * (chunks - 1) // 3)
            def _():
                run(f"c{quarter}")

    last = jnp.int32(chunks - 1)
    for shift in range(1, levels - 1):
        add_chunk(last, shift)
    receive(last, levels - 1)
    for ring in first:
        ring.finish()
    run("c3")

    scale = head_dim ** (-0.5)

    def prepare(step, normed):
        span = span_of(step)
        total = embedded[span, :] + picked(last, levels - 1, span)
        embedded[span, :] = total
        normed[...] = layer_norm(total).astype(bf16)

    def project(step, normed):
        span = span_of(step)
        queries[span, :] = dot_f32(normed[...], proj[0]).astype(bf16) * jnp.asarray(scale, bf16)
        keys[span, :] = dot_f32(normed[...], proj[1]).astype(bf16)
        found = dot_f32(normed[...], proj[2])
        for pair in range(heads // 2):
            turned = found[:, pair * LANES : (pair + 1) * LANES].T.astype(bf16)
            values_t[2 * pair, 0:head_dim, span] = turned[0:head_dim]
            values_t[2 * pair + 1, 0:head_dim, span] = turned[head_dim:]

    prepare(0, normed_a)

    @pl.loop(0, tiles // 2)
    def _(half):
        for quarter in range(2):
            @pl.when(half == min(1 + quarter, tiles // 2 - 1))
            def _():
                run(f"q{quarter}")

        step = 2 * half
        project(step, normed_a)
        prepare(step + 1, normed_b)

        project(step + 1, normed_b)

        @pl.when(half < tiles // 2 - 1)
        def _():
            prepare(step + 2, normed_a)

    def attended_copy(stage, shift, owner, target):
        owner_columns = pl.ds(pl.multiple_of(owner * columns, columns), columns)
        place = attended.at[span_of(stage), owner_columns]
        return pltpu.make_async_remote_copy(
            src_ref=place, dst_ref=place,
            send_sem=att_send.at[shift], recv_sem=att_recv.at[stage, shift],
            device_id={"level": target}, device_id_type=MESH,
        )

    def attended_out(stage, shift):
        return attended_copy(stage, shift, level, lax.rem(level + shift, levels))

    def attended_in(stage, shift):
        sender = lax.rem(level + levels - shift, levels)
        return attended_copy(stage, shift, sender, sender)

    lower = lax.broadcasted_iota(jnp.int32, (tile, LANES), 1) < head_dim
    part = frames // 2
    buffers = ((scores_a, peaks_a), (scores_b, peaks_b))

    def masked_query(stage, head):
        query = queries[span_of(stage), pl.ds(head // 2 * LANES, LANES)]
        zero = jnp.zeros_like(query)
        return jnp.where(lower, query, zero) if head % 2 == 0 else jnp.where(lower, zero, query)

    def score_part(query, head, buffer, begin, count):
        found = dot_nt(keys[begin : begin + count, head // 2 * LANES : (head // 2 + 1) * LANES], query)
        buffer[0][begin : begin + count, :] = found
        return jnp.max(found.reshape(count // 8, 8, tile), axis=0)

    def mix_part(head, buffer, peak, begin, count):
        weights = jnp.exp(buffer[0][begin : begin + count, :] - peak).astype(bf16)
        return dot_f32(values_t[head, :, begin : begin + count], weights)

    def attend(stage, head, buffer, next_stage, next_head, next_buffer):
        query = masked_query(next_stage, next_head)
        peak = jnp.max(buffer[1][...], axis=0, keepdims=True)
        top, mixed = [], []
        for begin in range(0, frames, part):
            top.append(score_part(query, next_head, next_buffer, begin, part))
            mixed.append(mix_part(head, buffer, peak, begin, part))
        next_buffer[1][...] = jnp.maximum(top[0], top[1])
        total = mixed[0] + mixed[1]
        return total[0:head_dim] * (1.0 / total[head_dim : head_dim + 1])

    peaks_a[...] = score_part(masked_query(0, 0), 0, buffers[0], 0, frames)

    @pl.loop(0, tiles)
    def _(stage):
        for sixth in range(6):
            @pl.when(stage == sixth * tiles // 6)
            def _():
                run(f"s{sixth}")

        @pl.when(stage > 0)
        def _():
            for shift in range(1, levels):
                attended_out(stage - 1, shift).start()

        low = None
        for head in range(heads):
            ahead = (stage, head + 1) if head + 1 < heads else (lax.min(stage + 1, tiles - 1), 0)
            found = attend(stage, head, buffers[head % 2], *ahead, buffers[(head + 1) % 2])
            if head % 2 == 0:
                low = found
            else:
                across = pl.ds(pl.multiple_of(level * columns + head // 2 * LANES, LANES), LANES)
                attended[span_of(stage), across] = jnp.concatenate([low, found], axis=0).T.astype(bf16)

    for shift in range(1, levels):
        attended_out(tiles - 1, shift).start()
    run("end")
    for ring in second:
        ring.finish()

    taps = depth_ref.shape[0]
    depth = depth_ref[...].astype(jnp.float32)

    def gate(step):
        for shift in range(1, levels):
            attended_in(step, shift).wait_recv()
        span = span_of(step)
        after_attn = embedded[span, :] + dot_nt(attended[span, :], rest[0])
        embedded[span, :] = after_attn
        normed = layer_norm(after_attn).astype(bf16)
        mixed = dot_f32(normed, rest[1]) * jax.nn.sigmoid(dot_f32(normed, rest[2]))
        gated[pl.ds(pl.multiple_of(PAD + step * tile, PAD), tile), :] = mixed.astype(bf16)

    def final_copy(step):
        span = span_of(step)
        return pltpu.make_async_copy(final.at[span], final_ref.at[span], final_sem.at[0])

    def convolve(step):
        span = span_of(step)
        start = pl.multiple_of(step * tile, tile)
        window = gated[pl.ds(start, tile + 2 * PAD), :].astype(jnp.float32)
        conv = jnp.zeros((tile, width), jnp.float32)
        for tap in range(taps):
            first_row = PAD - taps // 2 + tap
            conv = conv + window[first_row : first_row + tile] * depth[tap : tap + 1, :]
        activated = (conv * jax.nn.sigmoid(conv)).astype(bf16)
        after_conv = embedded[span, :] + dot_f32(activated, rest[3])
        final[span, :] = layer_norm(after_conv).astype(bf16)
        final_copy(step).start()

    gate(0)
    gate(1)

    @pl.loop(0, tiles - 2)
    def _(step):
        convolve(step)
        gate(step + 2)

    convolve(tiles - 2)
    convolve(tiles - 1)

    for shift in range(1, levels):
        for kind in range(4):
            over_level(kind, shift).wait_send()

        sent = tables.at[level, pl.ds(0, codes // CORES)]
        for kind in range(2):
            pltpu.make_async_remote_copy(
                src_ref=sent, dst_ref=sent,
                send_sem=table_send.at[kind, shift], recv_sem=table_recv.at[kind, shift, 0],
                device_id={"level": level}, device_id_type=MESH,
            ).wait_send()
        sent = attended.at[:, own_columns]
        pltpu.make_async_remote_copy(
            src_ref=sent, dst_ref=sent,
            send_sem=att_send.at[shift], recv_sem=att_recv.at[0, shift],
            device_id={"level": level}, device_id_type=MESH,
        ).wait_send()

    pltpu.make_async_copy(final, final_ref, final_sem.at[0]).wait()


def decode_step(levels, devices, tokens, decoded, done, fill, table, w_qkv, w_out_t, w_expand, w_project, taps):
    frames, width = tokens.shape[1], table.shape[1]
    chips = devices // CORES
    columns = width // levels
    chunks = table.shape[0] // (CORES * LANES)
    tiles = frames // (2 * LANES)
    vmem = pl.BlockSpec(memory_space=pltpu.VMEM)
    anywhere = pl.BlockSpec(memory_space=pl.ANY)
    dma = pltpu.SemaphoreType.DMA
    half = chips // 2
    bf16, f32 = jnp.bfloat16, jnp.float32
    return pl.pallas_call(
        functools.partial(step_kernel, levels, devices, frames, width),
        out_shape=jax.ShapeDtypeStruct((frames, width), bf16),
        in_specs=[anywhere] * 2 + [pl.BlockSpec(memory_space=pltpu.SMEM)] + [anywhere] * 6 + [vmem],
        out_specs=anywhere,
        scratch_shapes=[
            pltpu.VMEM((levels,) + tokens.shape, jnp.int32),
            pltpu.VMEM((levels,) + decoded.shape, jnp.int32),
            pltpu.VMEM((levels,) + fill.shape, bf16),
            pltpu.VMEM((levels, frames, LANES), f32),
            pltpu.VMEM((levels,) + table.shape, bf16),
            pltpu.VMEM((3, width, columns), bf16),
            pltpu.VMEM((4, width, width), bf16),
            pltpu.VMEM((frames, width), f32),
            pltpu.VMEM((frames, columns), bf16),
            pltpu.VMEM((columns // (width // HEADS), width // HEADS + 16, frames), bf16),
            pltpu.VMEM((frames, columns), bf16),
            pltpu.VMEM((2 * LANES, width), bf16),
            pltpu.VMEM((2 * LANES, width), bf16),
            pltpu.VMEM((frames, width), bf16),
            pltpu.VMEM((frames + 2 * PAD, width), bf16),
            pltpu.VMEM((frames, width), bf16),
            pltpu.VMEM((frames, 2 * LANES), f32),
            pltpu.VMEM((frames, 2 * LANES), f32),
            pltpu.VMEM((8, 2 * LANES), f32),
            pltpu.VMEM((8, 2 * LANES), f32),
            dma((11,)),
            dma((4, levels)), dma((4, levels)), dma((2, levels)), dma((2, levels, chunks)),
            dma((levels,)), dma((tiles, levels)), dma((1,)),
        ]
        + [
            dma(shape) for count in (3, 4) for shape in ((count,), (count, 2, half), (count,), (count,))
        ],
        compiler_params=pltpu.CompilerParams(
            collective_id=0, has_side_effects=True, vmem_limit_bytes=64000 * 1024
        ),
    )(tokens, decoded, done, fill, table, w_qkv, w_out_t, w_expand, w_project, taps)


def head_kernel(final_ref, head_ref, logits_ref):
    logits_ref[...] = dot_f32(final_ref[...], head_ref[...]).astype(logits_ref.dtype)


def score(final, head):
    frames, width = final.shape
    codes = head.shape[1]
    tile = 2 * LANES
    return pl.pallas_call(
        head_kernel,
        out_shape=jax.ShapeDtypeStruct((frames, codes), final.dtype),
        grid=(frames // tile,),
        in_specs=[pl.BlockSpec((tile, width), lambda step: (step, 0)), pl.BlockSpec((width, codes), lambda step: (0, 0))],
        out_specs=pl.BlockSpec((tile, codes), lambda step: (step, 0)),
    )(final, head)


def body(
    token_ids,
    decoded_mask,
    levels_done,
    code_tables,
    mask_vectors,
    w_qkv,
    w_out,
    w_expand,
    w_depth,
    w_project,
    level_heads,
):
    final = decode_step(
        lax.axis_size("level"), lax.axis_size("dp"), token_ids[0], decoded_mask[0], levels_done, mask_vectors,
        code_tables[0], w_qkv, w_out.T, w_expand, w_project, w_depth,
    )
    return score(final, level_heads[0])[None, None]


def solution(mesh):
    return jax.shard_map(
        body,
        mesh=mesh,
        in_specs=(
            P("dp", "level", None),
            P("dp", "level", None),
            P("dp"),
            P("level", None, None),
            P("level", None),
            P(None, "dp", "level"),
            P("level", "dp"),
            P("dp", None),
            P(),
            P("dp", None),
            P("level", None, None),
        ),
        out_specs=P("dp", "level", None, None),
        check_vma=False,
    )
```

```python
import functools

import jax
import jax.numpy as jnp
from jax import lax
from jax.experimental import pallas as pl
from jax.experimental.pallas import tpu as pltpu
from jax.sharding import PartitionSpec as P

HEADS = 16
CORES = 2
LANES = 128
PAD = 16
MESH = pl.DeviceIdType.MESH


def layer_norm(values):
    centered = values - jnp.mean(values, axis=-1, keepdims=True)
    variance = jnp.mean(centered * centered, axis=-1, keepdims=True)
    return centered * lax.rsqrt(variance + 1e-05)


def dot_f32(left, right):
    return jnp.dot(left, right, preferred_element_type=jnp.float32)


def dot_nt(left, right):
    return lax.dot_general(left, right, (((1,), (1,)), ((), ())), preferred_element_type=jnp.float32)


def chip_at(position, chips):
    position = lax.rem(position + 2 * chips, chips)
    turned = position // (chips // 2)
    return (1 - turned) * 2 * position + turned * (2 * (chips - 1 - position) + 1)


def position_of(chip, chips):
    odd = lax.rem(chip, 2)
    return (1 - odd) * (chip // 2) + odd * (chips - 1 - chip // 2)


class Ring:
    def __init__(self, full, own, rows, chips, sems):
        self.full, self.own, self.rows, self.chips, self.half = full, own, rows, chips, chips // 2
        self.send, self.recv, self.sib_send, self.sib_recv = sems
        self.device = lax.axis_index("dp")
        self.core = lax.rem(self.device, CORES)
        self.position = position_of(self.device // CORES, chips)

    def block(self, position, core, part):
        row = (chip_at(position, self.chips) * CORES + core) * self.rows
        count = self.rows
        if part is not None:
            count = self.rows // 2
            row = row + part * count
        return self.full.at[pl.ds(pl.multiple_of(row, count), count), :]

    def own_block(self, part):
        if self.own is None:
            return self.block(self.position, self.core, part)
        if part is None:
            return self.own
        count = self.rows // 2
        return self.own.at[pl.ds(part * count, count), :]

    def part(self, way, step):
        return way if step == self.half - 1 else None

    def origin(self, way, step):
        return self.position - (1 + step) if way == 0 else self.position + (1 + step)

    def hop(self, way, step):
        towards = self.position + 1 if way == 0 else self.position - 1
        source = self.position - step if way == 0 else self.position + step
        part = self.part(way, step)
        place = self.block(source, self.core, part)
        target = chip_at(towards, self.chips) * CORES + self.core
        return pltpu.make_async_remote_copy(
            src_ref=self.own_block(part) if step == 0 else place,
            dst_ref=place,
            send_sem=self.send,
            recv_sem=self.recv.at[way, step],
            device_id={"dp": target},
            device_id_type=MESH,
        )

    def arrival(self, way, step):
        ref = self.block(self.origin(way, step), self.core, self.part(way, step))
        return pltpu.make_async_remote_copy(
            src_ref=ref,
            dst_ref=ref,
            send_sem=self.send,
            recv_sem=self.recv.at[way, step],
            device_id={"dp": self.device},
            device_id_type=MESH,
        )

    def share(self, way, step, core):
        position = self.position if step < 0 else self.origin(way, step)
        place = self.block(position, core, None if step < 0 else self.part(way, step))
        sibling = self.device + 1 - 2 * self.core
        return pltpu.make_async_remote_copy(
            src_ref=self.own_block(None) if step < 0 else place,
            dst_ref=place,
            send_sem=self.sib_send,
            recv_sem=self.sib_recv,
            device_id={"dp": sibling},
            device_id_type=MESH,
        )

    def start(self):
        for way in range(2):
            self.hop(way, 0).start()
        self.share(0, -1, self.core).start()

    def advance(self, step):
        for way in range(2):
            self.arrival(way, step).wait_recv()
            if step + 1 < self.half:
                self.hop(way, step + 1).start()
            self.share(way, step, self.core).start()

    def all_of(self, blocks, send, recv):
        ref = self.full.at[pl.ds(0, blocks * self.rows), :]
        return pltpu.make_async_remote_copy(
            src_ref=ref,
            dst_ref=ref,
            send_sem=send,
            recv_sem=recv,
            device_id={"dp": self.device},
            device_id_type=MESH,
        )

    def finish(self):
        self.all_of(self.chips - 1, self.send, self.sib_recv).wait_send()
        shared = self.all_of(self.chips, self.sib_send, self.sib_recv)
        shared.wait_send()
        shared.wait_recv()


def step_kernel(
    levels, devices, frames, width,
    tok_ref, dec_ref, done_ref, fill_ref, table_ref, qkv_ref, out_ref, expand_ref, project_ref, depth_ref,
    final_ref,
    toks, decs, fills, ids, tables, proj, rest, embedded, keys, values_t, queries,
    normed_a, normed_b, attended, gated, final, scores_a, scores_b, peaks_a, peaks_b,
    local_sem, level_send, level_recv, table_send, table_recv, att_send, att_recv, final_sem,
    ring_a, ring_a_recv, sib_a, sib_a_recv, ring_b, ring_b_recv, sib_b, sib_b_recv,
):
    level = lax.axis_index("level")
    device = lax.axis_index("dp")
    core = lax.rem(device, CORES)
    sibling = device + 1 - 2 * core
    chips = devices // CORES
    rows = width // devices
    columns = width // levels
    codes = table_ref.shape[0]
    position = position_of(device // CORES, chips)
    bf16 = jnp.bfloat16

    barrier = pltpu.get_barrier_semaphore()
    for shift in range(1, levels):
        pl.semaphore_signal(barrier, inc=1, device_id={"level": lax.rem(level + shift, levels)}, device_id_type=MESH)
    for other in (
        sibling,
        chip_at(position + 1, chips) * CORES + core,
        chip_at(position - 1, chips) * CORES + core,
    ):
        pl.semaphore_signal(barrier, inc=1, device_id={"dp": other}, device_id_type=MESH)

    own_rows = pl.ds(pl.multiple_of(device * rows, rows), rows)
    own_columns = pl.ds(pl.multiple_of(level * columns, columns), columns)
    sources = (tok_ref, dec_ref, fill_ref, out_ref)

    def place_of(kind, owner):
        owner_columns = pl.ds(pl.multiple_of(owner * columns, columns), columns)
        return (toks.at[owner], decs.at[owner], fills.at[owner], rest.at[0, own_rows, owner_columns])[kind]

    def over_level(kind, shift):
        return pltpu.make_async_remote_copy(
            src_ref=sources[kind], dst_ref=place_of(kind, level),
            send_sem=level_send.at[kind, shift], recv_sem=level_recv.at[kind, shift],
            device_id={"level": lax.rem(level + shift, levels)}, device_id_type=MESH,
        )

    def from_level(kind, shift):
        sender = lax.rem(level + levels - shift, levels)
        return pltpu.make_async_remote_copy(
            src_ref=sources[kind], dst_ref=place_of(kind, sender),
            send_sem=level_send.at[kind, shift], recv_sem=level_recv.at[kind, shift],
            device_id={"level": sender}, device_id_type=MESH,
        )

    piece = LANES
    chunk = CORES * piece
    chunks = codes // chunk

    def chunk_rows(order, which):
        return pl.ds(pl.multiple_of((order * CORES + which) * piece, piece), piece)

    def table_out(order, shift):
        return pltpu.make_async_remote_copy(
            src_ref=table_ref.at[chunk_rows(order, core)], dst_ref=tables.at[level, chunk_rows(order, core)],
            send_sem=table_send.at[0, shift], recv_sem=table_recv.at[0, shift, order],
            device_id={"level": lax.rem(level + shift, levels)}, device_id_type=MESH,
        )

    def table_at(order, shift, which, kind):
        place = tables.at[lax.rem(level + levels - shift, levels), chunk_rows(order, which)]
        return pltpu.make_async_remote_copy(
            src_ref=place, dst_ref=place,
            send_sem=table_send.at[kind, shift], recv_sem=table_recv.at[kind, shift, order],
            device_id={"dp": sibling}, device_id_type=MESH,
        )

    early = [
        pltpu.make_async_copy(sources[kind], place_of(kind, level), local_sem.at[kind]) for kind in range(3)
    ] + [pltpu.make_async_copy(table_ref, tables.at[level], local_sem.at[3])]
    late = [
        pltpu.make_async_copy(qkv_ref.at[part], proj.at[part, own_rows, :], local_sem.at[4 + part]) for part in range(3)
    ] + [
        pltpu.make_async_copy(out_ref, place_of(3, level), local_sem.at[7]),
        pltpu.make_async_copy(expand_ref.at[:, pl.ds(0, width)], rest.at[1, own_rows, :], local_sem.at[8]),
        pltpu.make_async_copy(expand_ref.at[:, pl.ds(width, width)], rest.at[2, own_rows, :], local_sem.at[9]),
        pltpu.make_async_copy(project_ref, rest.at[3, own_rows, :], local_sem.at[10]),
    ]
    for copy in early + late:
        copy.start()

    def rings(full, own, count, sems):
        return [
            Ring(full.at[part], own(part), rows, chips, tuple(sem.at[part] for sem in sems))
            for part in range(count)
        ]

    first = rings(proj, lambda part: qkv_ref.at[part], 3, (ring_a, ring_a_recv, sib_a, sib_a_recv))
    rest_sources = (
        None, expand_ref.at[:, pl.ds(0, width)], expand_ref.at[:, pl.ds(width, width)], project_ref,
    )
    second = rings(rest, lambda part: rest_sources[part], 4, (ring_b, ring_b_recv, sib_b, sib_b_recv))
    hops = chips // 2
    turn = (1, 2, 0, 3)
    slots = ("c1", "c2", "c3", "q0", "q0", "q1", "s0", "s1", "s2", "s2", "s3", "s4", "s4", "s5", "s5", "end")
    plan = {}

    def at_slot(slot, act):
        plan.setdefault(slot, []).append(act)

    def run(slot):
        for act in plan.get(slot, ()):
            act()

    def start_second(part):
        if part == 0:
            for copy in late:
                copy.wait()
            for shift in range(1, levels):
                from_level(3, shift).wait_recv()
        second[part].start()

    for step in range(hops):
        slot = ("e", "c0", "c1", "c2")[step * 4 // hops]
        for ring in first:
            at_slot(slot, functools.partial(ring.advance, step))
    for slot, part in zip(("start", "e", "c0", "c1"), turn):
        at_slot(slot, functools.partial(start_second, part))
    order_of = [(step, part) for step in range(hops) for part in turn]
    for index, (step, part) in enumerate(order_of):
        at_slot(slots[index * len(slots) // len(order_of)], functools.partial(second[part].advance, step))

    pl.semaphore_wait(barrier, levels + 2)
    for kind in range(3):
        for shift in range(1, levels):
            over_level(kind, shift).start()
    for ring in first:
        ring.start()
    run("start")
    for shift in range(1, levels):
        over_level(3, shift).start()
    for order in range(chunks):
        for shift in range(1, levels):
            table_out(order, shift).start()

    head_dim = width // HEADS
    heads = columns // head_dim
    for head in range(heads):
        values_t[head, head_dim:, :] = jnp.ones((values_t.shape[1] - head_dim, frames), bf16)
    groups = width // LANES
    for place in (pl.ds(0, PAD), pl.ds(PAD + frames, PAD)):
        gated[:, place, :] = jnp.zeros((groups, PAD, LANES), jnp.float32)

    for copy in early:
        copy.wait()
    for kind in range(3):
        for shift in range(1, levels):
            from_level(kind, shift).wait_recv()

    done = done_ref[0]
    for row in range(levels):
        use = (row < done) | ((row == done) & (decs[row] == 1))
        code = jnp.where(use, toks[row], -1).astype(jnp.float32)
        for base in range(0, frames, LANES):
            ids[row, base : base + LANES, :] = jnp.broadcast_to(code[:, base : base + LANES], (LANES, LANES)).T

    tile = 2 * LANES
    tiles = frames // tile
    lane = lax.broadcasted_iota(jnp.int32, (tile, LANES), 1).astype(jnp.float32)

    def span_of(step):
        return pl.ds(step * tile if isinstance(step, int) else pl.multiple_of(step * tile, tile), tile)

    def onehot(found, start, count):
        return jnp.concatenate(
            [jnp.where(found - start == lane + float(base), 1.0, 0.0).astype(bf16) for base in range(0, count, LANES)],
            axis=1,
        )

    @pl.loop(0, tiles)
    def _(step):
        @pl.when(step == tiles // 2)
        def _():
            run("e")

        span = span_of(step)
        total = dot_f32(onehot(ids[level, span, :], 0.0, codes), tables[level])
        for row in range(levels):
            total = total + jnp.where(ids[row, span, 0:1] < 0.0, fills[row].astype(jnp.float32), 0.0)
        embedded[span, :] = total

    def receive(order, shift):
        table_at(order, shift, core, 0).wait_recv()
        table_at(order, shift, core, 1).start()
        table_at(order, shift, 1 - core, 1).wait_recv()

    def picked(order, shift, span):
        sender = lax.rem(level + levels - shift, levels)
        found = onehot(ids[sender, span, :], lax.convert_element_type(order * chunk, jnp.float32), chunk)
        return dot_f32(found, tables[sender, pl.ds(pl.multiple_of(order * chunk, chunk), chunk), :])

    def add_chunk(order, shift):
        receive(order, shift)

        @pl.loop(0, tiles)
        def _(step):
            span = span_of(step)
            embedded[span, :] = embedded[span, :] + picked(order, shift, span)

    @pl.loop(0, chunks - 1)
    def _(order):
        for shift in range(1, levels):
            add_chunk(order, shift)
        for quarter in range(3):
            @pl.when(order == quarter * (chunks - 1) // 3)
            def _():
                run(f"c{quarter}")

    last = jnp.int32(chunks - 1)
    for shift in range(1, levels - 1):
        add_chunk(last, shift)
    receive(last, levels - 1)
    for ring in first:
        ring.finish()
    run("c3")

    scale = head_dim ** (-0.5)

    wide = 2 * tile
    units = frames // wide

    def prepare(unit, normed):
        span = pl.ds(unit * wide, wide)
        total = embedded[span, :] + jnp.concatenate(
            [picked(last, levels - 1, span_of(2 * unit + half)) for half in range(2)], axis=0
        )
        embedded[span, :] = total
        normed[...] = layer_norm(total).astype(bf16)

    def project(unit, normed):
        span = pl.ds(unit * wide, wide)
        queries[span, :] = dot_f32(normed[...], proj[0]).astype(bf16) * jnp.asarray(scale, bf16)
        keys[span, :] = dot_f32(normed[...], proj[1]).astype(bf16)
        found = dot_f32(normed[...], proj[2])
        for pair in range(heads // 2):
            turned = found[:, pair * LANES : (pair + 1) * LANES].T.astype(bf16)
            values_t[2 * pair, 0:head_dim, span] = turned[0:head_dim]
            values_t[2 * pair + 1, 0:head_dim, span] = turned[head_dim:]

    spare = (normed_a, normed_b)
    prepare(0, normed_a)
    for unit in range(units):
        project(unit, spare[unit % 2])
        if unit + 1 < units:
            prepare(unit + 1, spare[(unit + 1) % 2])
            if unit + 2 == units:
                run("q1")
            elif unit == 0:
                run("q0")

    pairs = heads // 2

    def pieces_of(stage):
        if isinstance(stage, int) and stage == 0:
            return [(pair, pair * LANES, LANES) for pair in range(pairs)]
        return [(stage + pairs - 1, 0, columns)]

    def attended_copy(stage, piece, shift, owner, target):
        index, start, count = piece
        place = attended.at[span_of(stage), pl.ds(pl.multiple_of(owner * columns + start, LANES), count)]
        return pltpu.make_async_remote_copy(
            src_ref=place, dst_ref=place,
            send_sem=att_send.at[shift], recv_sem=att_recv.at[index, shift],
            device_id={"level": target}, device_id_type=MESH,
        )

    def attended_out(stage, piece, shift):
        return attended_copy(stage, piece, shift, level, lax.rem(level + shift, levels))

    def attended_in(stage, piece, shift):
        sender = lax.rem(level + levels - shift, levels)
        return attended_copy(stage, piece, shift, sender, sender)

    lower = lax.broadcasted_iota(jnp.int32, (tile, LANES), 1) < head_dim
    part = frames // 2
    buffers = ((scores_a, peaks_a), (scores_b, peaks_b))

    def masked_query(stage, head):
        query = queries[span_of(stage), pl.ds(head // 2 * LANES, LANES)]
        zero = jnp.zeros_like(query)
        return jnp.where(lower, query, zero) if head % 2 == 0 else jnp.where(lower, zero, query)

    def score_part(query, head, buffer, begin, count):
        found = dot_nt(keys[begin : begin + count, head // 2 * LANES : (head // 2 + 1) * LANES], query)
        buffer[0][begin : begin + count, :] = found
        return jnp.max(found.reshape(count // 8, 8, tile), axis=0)

    def mix_part(head, buffer, peak, begin, count):
        weights = jnp.exp(buffer[0][begin : begin + count, :] - peak).astype(bf16)
        return dot_f32(values_t[head, :, begin : begin + count], weights)

    def attend(stage, head, buffer, next_stage, next_head, next_buffer):
        query = masked_query(next_stage, next_head)
        peak = jnp.max(buffer[1][...], axis=0, keepdims=True)
        top, mixed = [], []
        for begin in range(0, frames, part):
            top.append(score_part(query, next_head, next_buffer, begin, part))
            mixed.append(mix_part(head, buffer, peak, begin, part))
        next_buffer[1][...] = jnp.maximum(top[0], top[1])
        total = mixed[0] + mixed[1]
        return total[0:head_dim] * (1.0 / total[head_dim : head_dim + 1])

    peaks_a[...] = score_part(masked_query(0, 0), 0, buffers[0], 0, frames)

    def attend_all(stage):
        pieces = pieces_of(stage)
        low = None
        for head in range(heads):
            ahead = (stage, head + 1) if head + 1 < heads else (lax.min(stage + 1, tiles - 1), 0)
            found = attend(stage, head, buffers[head % 2], *ahead, buffers[(head + 1) % 2])
            if head % 2 == 0:
                low = found
            else:
                across = pl.ds(pl.multiple_of(level * columns + head // 2 * LANES, LANES), LANES)
                attended[span_of(stage), across] = jnp.concatenate([low, found], axis=0).T.astype(bf16)
                if (head + 1) * len(pieces) % heads == 0:
                    for shift in range(1, levels):
                        attended_out(stage, pieces[(head + 1) * len(pieces) // heads - 1], shift).start()

    run("s0")
    attend_all(0)

    @pl.loop(1, tiles)
    def _(stage):
        for sixth in range(1, 6):
            @pl.when(stage == sixth * tiles // 6)
            def _():
                run(f"s{sixth}")

        attend_all(stage)

    run("end")
    for part in turn[:-1]:
        second[part].finish()

    taps = depth_ref.shape[0]
    depth = depth_ref[...].astype(jnp.float32)

    def gate(step, count):
        for ahead in range(count):
            for piece in pieces_of(step + ahead):
                for shift in range(1, levels):
                    attended_in(step + ahead, piece, shift).wait_recv()
        span = pl.ds(step * tile, count * tile)
        after_attn = embedded[span, :] + dot_nt(attended[span, :], rest[0])
        embedded[span, :] = after_attn
        normed = layer_norm(after_attn).astype(bf16)
        mixed = dot_f32(normed, rest[1]) * jax.nn.sigmoid(dot_f32(normed, rest[2]))
        mixed = mixed.astype(bf16).astype(jnp.float32)
        for group in range(groups):
            gated[group, pl.ds(PAD + step * tile, count * tile), :] = mixed[:, group * LANES : (group + 1) * LANES]

    def final_copy(step):
        span = span_of(step)
        return pltpu.make_async_copy(final.at[span], final_ref.at[span], final_sem.at[0])

    def convolve(step):
        span = span_of(step)
        conv = []
        for group in range(groups):
            across = slice(group * LANES, (group + 1) * LANES)
            terms = [
                gated[group, pl.ds(step * tile + (PAD - taps // 2 + tap), tile), :] * depth[tap : tap + 1, across]
                for tap in range(taps)
            ]
            conv.append(functools.reduce(jnp.add, terms))
        conv = jnp.concatenate(conv, axis=1)
        activated = (conv * jax.nn.sigmoid(conv)).astype(bf16)
        after_conv = embedded[span, :] + dot_f32(activated, rest[3])
        final[span, :] = layer_norm(after_conv).astype(bf16)
        final_copy(step).start()

    ready = convolved = 0
    while convolved < tiles:
        if ready < tiles:
            count = 2 if ready + 4 <= tiles else 1
            gate(ready, count)
            if ready == 0:
                second[turn[-1]].finish()
            ready += count
        limit = tiles if ready == tiles else ready - 1
        while convolved < limit:
            convolve(convolved)
            convolved += 1

    for shift in range(1, levels):
        for kind in range(4):
            over_level(kind, shift).wait_send()

        sent = tables.at[level, pl.ds(0, codes // CORES)]
        for kind in range(2):
            pltpu.make_async_remote_copy(
                src_ref=sent, dst_ref=sent,
                send_sem=table_send.at[kind, shift], recv_sem=table_recv.at[kind, shift, 0],
                device_id={"level": level}, device_id_type=MESH,
            ).wait_send()
        sent = attended.at[:, own_columns]
        pltpu.make_async_remote_copy(
            src_ref=sent, dst_ref=sent,
            send_sem=att_send.at[shift], recv_sem=att_recv.at[0, shift],
            device_id={"level": level}, device_id_type=MESH,
        ).wait_send()

    pltpu.make_async_copy(final, final_ref, final_sem.at[0]).wait()


def decode_step(levels, devices, tokens, decoded, done, fill, table, w_qkv, w_out_t, w_expand, w_project, taps):
    frames, width = tokens.shape[1], table.shape[1]
    chips = devices // CORES
    columns = width // levels
    chunks = table.shape[0] // (CORES * LANES)
    tiles = frames // (2 * LANES)
    vmem = pl.BlockSpec(memory_space=pltpu.VMEM)
    anywhere = pl.BlockSpec(memory_space=pl.ANY)
    dma = pltpu.SemaphoreType.DMA
    half = chips // 2
    bf16, f32 = jnp.bfloat16, jnp.float32
    return pl.pallas_call(
        functools.partial(step_kernel, levels, devices, frames, width),
        out_shape=jax.ShapeDtypeStruct((frames, width), bf16),
        in_specs=[anywhere] * 2 + [pl.BlockSpec(memory_space=pltpu.SMEM)] + [anywhere] * 6 + [vmem],
        out_specs=anywhere,
        scratch_shapes=[
            pltpu.VMEM((levels,) + tokens.shape, jnp.int32),
            pltpu.VMEM((levels,) + decoded.shape, jnp.int32),
            pltpu.VMEM((levels,) + fill.shape, bf16),
            pltpu.VMEM((levels, frames, LANES), f32),
            pltpu.VMEM((levels,) + table.shape, bf16),
            pltpu.VMEM((3, width, columns), bf16),
            pltpu.VMEM((4, width, width), bf16),
            pltpu.VMEM((frames, width), f32),
            pltpu.VMEM((frames, columns), bf16),
            pltpu.VMEM((columns // (width // HEADS), width // HEADS + 16, frames), bf16),
            pltpu.VMEM((frames, columns), bf16),
            pltpu.VMEM((4 * LANES, width), bf16),
            pltpu.VMEM((4 * LANES, width), bf16),
            pltpu.VMEM((frames, width), bf16),
            pltpu.VMEM((width // LANES, frames + 2 * PAD, LANES), f32),
            pltpu.VMEM((frames, width), bf16),
            pltpu.VMEM((frames, 2 * LANES), f32),
            pltpu.VMEM((frames, 2 * LANES), f32),
            pltpu.VMEM((8, 2 * LANES), f32),
            pltpu.VMEM((8, 2 * LANES), f32),
            dma((11,)),
            dma((4, levels)), dma((4, levels)), dma((2, levels)), dma((2, levels, chunks)),
            dma((levels,)), dma((tiles + columns // LANES - 1, levels)), dma((1,)),
        ]
        + [
            dma(shape) for count in (3, 4) for shape in ((count,), (count, 2, half), (count,), (count,))
        ],
        compiler_params=pltpu.CompilerParams(
            collective_id=0, has_side_effects=True, vmem_limit_bytes=64000 * 1024
        ),
    )(tokens, decoded, done, fill, table, w_qkv, w_out_t, w_expand, w_project, taps)


def head_kernel(parts, final_ref, head_ref, logits_ref, final, head, logits, final_sem, head_sem, logits_sem):
    rows, columns = final.shape[0] // parts, head.shape[1] // 2
    spans = [pl.ds(part * rows, rows) for part in range(parts)]
    sides = [pl.ds(side * columns, columns) for side in range(2)]
    finals = [pltpu.make_async_copy(final_ref.at[span], final.at[span], final_sem.at[i]) for i, span in enumerate(spans)]
    heads = [pltpu.make_async_copy(head_ref.at[:, side], head.at[:, side], head_sem.at[i]) for i, side in enumerate(sides)]
    outs = [pltpu.make_async_copy(logits.at[span], logits_ref.at[span], logits_sem.at[i]) for i, span in enumerate(spans)]
    for copy in finals[:1] + heads + finals[1:]:
        copy.start()
    for part, span in enumerate(spans):
        finals[part].wait()
        for which, side in enumerate(sides):
            if part == 0:
                heads[which].wait()
            logits[span, side] = dot_f32(final[span, :], head[:, side]).astype(logits.dtype)
        outs[part].start()
    for copy in outs:
        copy.wait()


def score(final, head):
    frames, codes = final.shape[0], head.shape[1]
    parts = 3
    hbm = pl.BlockSpec(memory_space=pltpu.HBM)
    dma = pltpu.SemaphoreType.DMA
    return pl.pallas_call(
        functools.partial(head_kernel, parts),
        out_shape=jax.ShapeDtypeStruct((frames, codes), final.dtype),
        in_specs=[hbm, hbm],
        out_specs=hbm,
        scratch_shapes=[
            pltpu.VMEM(final.shape, final.dtype), pltpu.VMEM(head.shape, head.dtype),
            pltpu.VMEM((frames, codes), final.dtype), dma((parts,)), dma((2,)), dma((parts,)),
        ],
    )(final, head)


def body(
    token_ids,
    decoded_mask,
    levels_done,
    code_tables,
    mask_vectors,
    w_qkv,
    w_out,
    w_expand,
    w_depth,
    w_project,
    level_heads,
):
    final = decode_step(
        lax.axis_size("level"), lax.axis_size("dp"), token_ids[0], decoded_mask[0], levels_done, mask_vectors,
        code_tables[0], w_qkv, w_out.T, w_expand, w_project, w_depth,
    )
    return score(final, level_heads[0])[None, None]


def solution(mesh):
    return jax.shard_map(
        body,
        mesh=mesh,
        in_specs=(
            P("dp", "level", None),
            P("dp", "level", None),
            P("dp"),
            P("level", None, None),
            P("level", None),
            P(None, "dp", "level"),
            P("level", "dp"),
            P("dp", None),
            P(),
            P("dp", None),
            P("level", None, None),
        ),
        out_specs=P("dp", "level", None, None),
        check_vma=False,
    )
```

```python
import functools

import jax
import jax.numpy as jnp
from jax import lax
from jax.experimental import pallas as pl
from jax.experimental.pallas import tpu as pltpu
from jax.sharding import PartitionSpec as P

HEADS = 16
CORES = 2
LANES = 128
PAD = 16
MESH = pl.DeviceIdType.MESH


def layer_norm(values):
    centered = values - jnp.mean(values, axis=-1, keepdims=True)
    variance = jnp.mean(centered * centered, axis=-1, keepdims=True)
    return centered * lax.rsqrt(variance + 1e-05)


def dot_f32(left, right):
    return jnp.dot(left, right, preferred_element_type=jnp.float32)


def dot_nt(left, right):
    return lax.dot_general(left, right, (((1,), (1,)), ((), ())), preferred_element_type=jnp.float32)


def chip_at(position, chips):
    position = lax.rem(position + 2 * chips, chips)
    turned = position // (chips // 2)
    return (1 - turned) * 2 * position + turned * (2 * (chips - 1 - position) + 1)


def position_of(chip, chips):
    odd = lax.rem(chip, 2)
    return (1 - odd) * (chip // 2) + odd * (chips - 1 - chip // 2)


class Ring:
    def __init__(self, full, own, rows, chips, sems):
        self.full, self.own, self.rows, self.chips, self.half = full, own, rows, chips, chips // 2
        self.send, self.recv, self.sib_send, self.sib_recv = sems
        self.device = lax.axis_index("dp")
        self.core = lax.rem(self.device, CORES)
        self.position = position_of(self.device // CORES, chips)

    def block(self, position, core, part):
        row = (chip_at(position, self.chips) * CORES + core) * self.rows
        count = self.rows
        if part is not None:
            count = self.rows // 2
            row = row + part * count
        return self.full.at[pl.ds(pl.multiple_of(row, count), count), :]

    def own_block(self, part):
        if self.own is None:
            return self.block(self.position, self.core, part)
        if part is None:
            return self.own
        count = self.rows // 2
        return self.own.at[pl.ds(part * count, count), :]

    def part(self, way, step):
        return way if step == self.half - 1 else None

    def origin(self, way, step):
        return self.position - (1 + step) if way == 0 else self.position + (1 + step)

    def hop(self, way, step):
        towards = self.position + 1 if way == 0 else self.position - 1
        source = self.position - step if way == 0 else self.position + step
        part = self.part(way, step)
        place = self.block(source, self.core, part)
        target = chip_at(towards, self.chips) * CORES + self.core
        return pltpu.make_async_remote_copy(
            src_ref=self.own_block(part) if step == 0 else place,
            dst_ref=place,
            send_sem=self.send,
            recv_sem=self.recv.at[way, step],
            device_id={"dp": target},
            device_id_type=MESH,
        )

    def arrival(self, way, step):
        ref = self.block(self.origin(way, step), self.core, self.part(way, step))
        return pltpu.make_async_remote_copy(
            src_ref=ref,
            dst_ref=ref,
            send_sem=self.send,
            recv_sem=self.recv.at[way, step],
            device_id={"dp": self.device},
            device_id_type=MESH,
        )

    def share(self, way, step, core):
        position = self.position if step < 0 else self.origin(way, step)
        place = self.block(position, core, None if step < 0 else self.part(way, step))
        sibling = self.device + 1 - 2 * self.core
        return pltpu.make_async_remote_copy(
            src_ref=self.own_block(None) if step < 0 else place,
            dst_ref=place,
            send_sem=self.sib_send,
            recv_sem=self.sib_recv,
            device_id={"dp": sibling},
            device_id_type=MESH,
        )

    def start(self):
        for way in range(2):
            self.hop(way, 0).start()
        self.share(0, -1, self.core).start()

    def advance(self, step):
        for way in range(2):
            self.arrival(way, step).wait_recv()
            if step + 1 < self.half:
                self.hop(way, step + 1).start()
            self.share(way, step, self.core).start()

    def all_of(self, blocks, send, recv):
        ref = self.full.at[pl.ds(0, blocks * self.rows), :]
        return pltpu.make_async_remote_copy(
            src_ref=ref,
            dst_ref=ref,
            send_sem=send,
            recv_sem=recv,
            device_id={"dp": self.device},
            device_id_type=MESH,
        )

    def finish(self):
        self.all_of(self.chips - 1, self.send, self.sib_recv).wait_send()
        shared = self.all_of(self.chips, self.sib_send, self.sib_recv)
        shared.wait_send()
        shared.wait_recv()


def step_kernel(
    levels, devices, frames, width,
    tok_ref, dec_ref, done_ref, fill_ref, table_ref, qkv_ref, out_ref, expand_ref, project_ref, depth_ref,
    final_ref,
    toks, decs, fills, ids, tables, proj, rest, embedded, keys, values_t, queries,
    normed_a, normed_b, attended, gated, final, scores_a, scores_b, peaks_a, peaks_b,
    local_sem, level_send, level_recv, table_send, table_recv, att_send, att_recv, final_sem,
    ring_a, ring_a_recv, sib_a, sib_a_recv, ring_b, ring_b_recv, sib_b, sib_b_recv,
):
    level = lax.axis_index("level")
    device = lax.axis_index("dp")
    core = lax.rem(device, CORES)
    sibling = device + 1 - 2 * core
    chips = devices // CORES
    rows = width // devices
    columns = width // levels
    codes = table_ref.shape[0]
    position = position_of(device // CORES, chips)
    bf16 = jnp.bfloat16

    barrier = pltpu.get_barrier_semaphore()
    for shift in range(1, levels):
        pl.semaphore_signal(barrier, inc=1, device_id={"level": lax.rem(level + shift, levels)}, device_id_type=MESH)
    for other in (
        sibling,
        chip_at(position + 1, chips) * CORES + core,
        chip_at(position - 1, chips) * CORES + core,
    ):
        pl.semaphore_signal(barrier, inc=1, device_id={"dp": other}, device_id_type=MESH)

    own_rows = pl.ds(pl.multiple_of(device * rows, rows), rows)
    own_columns = pl.ds(pl.multiple_of(level * columns, columns), columns)
    sources = (tok_ref, dec_ref, fill_ref, out_ref)

    def place_of(kind, owner):
        owner_columns = pl.ds(pl.multiple_of(owner * columns, columns), columns)
        return (toks.at[owner], decs.at[owner], fills.at[owner], rest.at[0, own_rows, owner_columns])[kind]

    def over_level(kind, shift):
        return pltpu.make_async_remote_copy(
            src_ref=sources[kind], dst_ref=place_of(kind, level),
            send_sem=level_send.at[kind, shift], recv_sem=level_recv.at[kind, shift],
            device_id={"level": lax.rem(level + shift, levels)}, device_id_type=MESH,
        )

    def from_level(kind, shift):
        sender = lax.rem(level + levels - shift, levels)
        return pltpu.make_async_remote_copy(
            src_ref=sources[kind], dst_ref=place_of(kind, sender),
            send_sem=level_send.at[kind, shift], recv_sem=level_recv.at[kind, shift],
            device_id={"level": sender}, device_id_type=MESH,
        )

    piece = LANES
    chunk = CORES * piece
    chunks = codes // chunk

    def chunk_rows(order, which):
        return pl.ds(pl.multiple_of((order * CORES + which) * piece, piece), piece)

    def table_out(order, shift):
        return pltpu.make_async_remote_copy(
            src_ref=table_ref.at[chunk_rows(order, core)], dst_ref=tables.at[level, chunk_rows(order, core)],
            send_sem=table_send.at[0, shift], recv_sem=table_recv.at[0, shift, order],
            device_id={"level": lax.rem(level + shift, levels)}, device_id_type=MESH,
        )

    def table_at(order, shift, which, kind):
        place = tables.at[lax.rem(level + levels - shift, levels), chunk_rows(order, which)]
        return pltpu.make_async_remote_copy(
            src_ref=place, dst_ref=place,
            send_sem=table_send.at[kind, shift], recv_sem=table_recv.at[kind, shift, order],
            device_id={"dp": sibling}, device_id_type=MESH,
        )

    early = [
        pltpu.make_async_copy(sources[kind], place_of(kind, level), local_sem.at[kind]) for kind in range(3)
    ] + [pltpu.make_async_copy(table_ref, tables.at[level], local_sem.at[3])]
    late = [
        pltpu.make_async_copy(qkv_ref.at[part], proj.at[part, own_rows, :], local_sem.at[4 + part]) for part in range(3)
    ] + [
        pltpu.make_async_copy(out_ref, place_of(3, level), local_sem.at[7]),
        pltpu.make_async_copy(expand_ref.at[:, pl.ds(0, width)], rest.at[1, own_rows, :], local_sem.at[8]),
        pltpu.make_async_copy(expand_ref.at[:, pl.ds(width, width)], rest.at[2, own_rows, :], local_sem.at[9]),
        pltpu.make_async_copy(project_ref, rest.at[3, own_rows, :], local_sem.at[10]),
    ]
    for copy in early + late:
        copy.start()

    def rings(full, own, count, sems):
        return [
            Ring(full.at[part], own(part), rows, chips, tuple(sem.at[part] for sem in sems))
            for part in range(count)
        ]

    first = rings(proj, lambda part: qkv_ref.at[part], 3, (ring_a, ring_a_recv, sib_a, sib_a_recv))
    rest_sources = (
        None, expand_ref.at[:, pl.ds(0, width)], expand_ref.at[:, pl.ds(width, width)], project_ref,
    )
    second = rings(rest, lambda part: rest_sources[part], 4, (ring_b, ring_b_recv, sib_b, sib_b_recv))
    hops = chips // 2
    turn = (1, 2, 0, 3)
    slots = ("c1", "c2", "c3", "q0", "q0", "q1", "s0", "s1", "s2", "s3", "s3", "s4", "s5", "s5", "end", "end")
    plan = {}

    def at_slot(slot, act):
        plan.setdefault(slot, []).append(act)

    def run(slot):
        for act in plan.get(slot, ()):
            act()

    def start_second(part):
        if part == 0:
            for copy in late:
                copy.wait()
            for shift in range(1, levels):
                from_level(3, shift).wait_recv()
        second[part].start()

    for step in range(hops):
        slot = ("e", "c0", "c1", "c2")[step * 4 // hops]
        for ring in first:
            at_slot(slot, functools.partial(ring.advance, step))
    for slot, part in zip(("start", "e", "c0", "c1"), turn):
        at_slot(slot, functools.partial(start_second, part))
    order_of = [(step, part) for step in range(hops) for part in turn]
    for index, (step, part) in enumerate(order_of):
        at_slot(slots[index * len(slots) // len(order_of)], functools.partial(second[part].advance, step))

    pl.semaphore_wait(barrier, levels + 2)
    for kind in range(3):
        for shift in range(1, levels):
            over_level(kind, shift).start()
    for ring in first:
        ring.start()
    run("start")
    for shift in range(1, levels):
        over_level(3, shift).start()
    for order in range(chunks):
        for shift in range(1, levels):
            table_out(order, shift).start()

    head_dim = width // HEADS
    heads = columns // head_dim
    for head in range(heads):
        values_t[head, head_dim:, :] = jnp.ones((values_t.shape[1] - head_dim, frames), bf16)
    groups = width // LANES
    for place in (pl.ds(0, PAD), pl.ds(PAD + frames, PAD)):
        gated[:, place, :] = jnp.zeros((groups, PAD, LANES), jnp.float32)

    for copy in early:
        copy.wait()
    for kind in range(3):
        for shift in range(1, levels):
            from_level(kind, shift).wait_recv()

    done = done_ref[0]
    for row in range(levels):
        use = (row < done) | ((row == done) & (decs[row] == 1))
        code = jnp.where(use, toks[row], -1).astype(jnp.float32)
        for base in range(0, frames, LANES):
            ids[row, base : base + LANES, :] = jnp.broadcast_to(code[:, base : base + LANES], (LANES, LANES)).T

    tile = 2 * LANES
    tiles = frames // tile
    lane = lax.broadcasted_iota(jnp.int32, (tile, LANES), 1).astype(jnp.float32)

    def span_of(step):
        return pl.ds(step * tile if isinstance(step, int) else pl.multiple_of(step * tile, tile), tile)

    def onehot(found, start, count):
        return jnp.concatenate(
            [jnp.where(found - start == lane + float(base), 1.0, 0.0).astype(bf16) for base in range(0, count, LANES)],
            axis=1,
        )

    @pl.loop(0, tiles)
    def _(step):
        @pl.when(step == tiles // 2)
        def _():
            run("e")

        span = span_of(step)
        total = dot_f32(onehot(ids[level, span, :], 0.0, codes), tables[level])
        for row in range(levels):
            total = total + jnp.where(ids[row, span, 0:1] < 0.0, fills[row].astype(jnp.float32), 0.0)
        embedded[span, :] = total

    def receive(order, shift):
        table_at(order, shift, core, 0).wait_recv()
        table_at(order, shift, core, 1).start()
        table_at(order, shift, 1 - core, 1).wait_recv()

    def picked(order, shift, span):
        sender = lax.rem(level + levels - shift, levels)
        found = onehot(ids[sender, span, :], lax.convert_element_type(order * chunk, jnp.float32), chunk)
        return dot_f32(found, tables[sender, pl.ds(pl.multiple_of(order * chunk, chunk), chunk), :])

    def add_chunk(order, shift):
        receive(order, shift)

        @pl.loop(0, tiles)
        def _(step):
            span = span_of(step)
            embedded[span, :] = embedded[span, :] + picked(order, shift, span)

    @pl.loop(0, chunks - 1)
    def _(order):
        for shift in range(1, levels):
            add_chunk(order, shift)
        for quarter in range(3):
            @pl.when(order == quarter * (chunks - 1) // 3)
            def _():
                run(f"c{quarter}")

    last = jnp.int32(chunks - 1)
    for shift in range(1, levels - 1):
        add_chunk(last, shift)
    receive(last, levels - 1)
    for ring in first:
        ring.finish()
    run("c3")

    scale = head_dim ** (-0.5)

    wide = 2 * tile
    units = frames // wide

    def prepare(unit, normed):
        span = pl.ds(unit * wide, wide)
        total = embedded[span, :] + jnp.concatenate(
            [picked(last, levels - 1, span_of(2 * unit + half)) for half in range(2)], axis=0
        )
        embedded[span, :] = total
        normed[...] = layer_norm(total).astype(bf16)

    def project(unit, normed):
        span = pl.ds(unit * wide, wide)
        queries[span, :] = dot_f32(normed[...], proj[0]).astype(bf16) * jnp.asarray(scale, bf16)
        keys[span, :] = dot_f32(normed[...], proj[1]).astype(bf16)
        found = dot_f32(normed[...], proj[2])
        for pair in range(heads // 2):
            turned = found[:, pair * LANES : (pair + 1) * LANES].T.astype(bf16)
            values_t[2 * pair, 0:head_dim, span] = turned[0:head_dim]
            values_t[2 * pair + 1, 0:head_dim, span] = turned[head_dim:]

    spare = (normed_a, normed_b)
    prepare(0, normed_a)
    for unit in range(units):
        project(unit, spare[unit % 2])
        if unit + 1 < units:
            prepare(unit + 1, spare[(unit + 1) % 2])
            if unit + 2 == units:
                run("q1")
            elif unit == 0:
                run("q0")

    pairs = heads // 2

    def pieces_of(stage):
        if isinstance(stage, int) and stage == 0:
            return [(pair, pair * LANES, LANES) for pair in range(pairs)]
        return [(stage + pairs - 1, 0, columns)]

    def attended_copy(stage, piece, shift, owner, target):
        index, start, count = piece
        place = attended.at[span_of(stage), pl.ds(pl.multiple_of(owner * columns + start, LANES), count)]
        return pltpu.make_async_remote_copy(
            src_ref=place, dst_ref=place,
            send_sem=att_send.at[shift], recv_sem=att_recv.at[index, shift],
            device_id={"level": target}, device_id_type=MESH,
        )

    def attended_out(stage, piece, shift):
        return attended_copy(stage, piece, shift, level, lax.rem(level + shift, levels))

    def attended_in(stage, piece, shift):
        sender = lax.rem(level + levels - shift, levels)
        return attended_copy(stage, piece, shift, sender, sender)

    lower = lax.broadcasted_iota(jnp.int32, (tile, LANES), 1) < head_dim
    part = frames // 2
    buffers = ((scores_a, peaks_a), (scores_b, peaks_b))

    def masked_query(stage, head):
        query = queries[span_of(stage), pl.ds(head // 2 * LANES, LANES)]
        zero = jnp.zeros_like(query)
        return jnp.where(lower, query, zero) if head % 2 == 0 else jnp.where(lower, zero, query)

    def score_part(query, head, buffer, begin, count):
        found = dot_nt(keys[begin : begin + count, head // 2 * LANES : (head // 2 + 1) * LANES], query)
        buffer[0][begin : begin + count, :] = found
        return jnp.max(found.reshape(count // 8, 8, tile), axis=0)

    def mix_part(head, buffer, peak, begin, count):
        weights = jnp.exp(buffer[0][begin : begin + count, :] - peak).astype(bf16)
        return dot_f32(values_t[head, :, begin : begin + count], weights)

    def attend(stage, head, buffer, next_stage, next_head, next_buffer):
        query = masked_query(next_stage, next_head)
        peak = jnp.max(buffer[1][...], axis=0, keepdims=True)
        top, mixed = [], []
        for begin in range(0, frames, part):
            top.append(score_part(query, next_head, next_buffer, begin, part))
            mixed.append(mix_part(head, buffer, peak, begin, part))
        next_buffer[1][...] = jnp.maximum(top[0], top[1])
        total = mixed[0] + mixed[1]
        return total[0:head_dim] * (1.0 / total[head_dim : head_dim + 1])

    peaks_a[...] = score_part(masked_query(0, 0), 0, buffers[0], 0, frames)

    def attend_all(stage):
        pieces = pieces_of(stage)
        low = None
        for head in range(heads):
            ahead = (stage, head + 1) if head + 1 < heads else (lax.min(stage + 1, tiles - 1), 0)
            found = attend(stage, head, buffers[head % 2], *ahead, buffers[(head + 1) % 2])
            if head % 2 == 0:
                low = found
            else:
                across = pl.ds(pl.multiple_of(level * columns + head // 2 * LANES, LANES), LANES)
                attended[span_of(stage), across] = jnp.concatenate([low, found], axis=0).T.astype(bf16)
                if (head + 1) * len(pieces) % heads == 0:
                    for shift in range(1, levels):
                        attended_out(stage, pieces[(head + 1) * len(pieces) // heads - 1], shift).start()

    run("s0")
    attend_all(0)

    @pl.loop(1, tiles)
    def _(stage):
        for sixth in range(1, 6):
            @pl.when(stage == sixth * tiles // 6)
            def _():
                run(f"s{sixth}")

        attend_all(stage)

    run("end")
    for part in turn[:-1]:
        second[part].finish()

    taps = depth_ref.shape[0]
    depth = depth_ref[...].astype(jnp.float32)

    def gate(step, count):
        for ahead in range(count):
            for piece in pieces_of(step + ahead):
                for shift in range(1, levels):
                    attended_in(step + ahead, piece, shift).wait_recv()
        span = pl.ds(step * tile, count * tile)
        after_attn = embedded[span, :] + dot_nt(attended[span, :], rest[0])
        embedded[span, :] = after_attn
        normed = layer_norm(after_attn).astype(bf16)
        mixed = dot_f32(normed, rest[1]) * jax.nn.sigmoid(dot_f32(normed, rest[2]))
        mixed = mixed.astype(bf16).astype(jnp.float32)
        for group in range(groups):
            gated[group, pl.ds(PAD + step * tile, count * tile), :] = mixed[:, group * LANES : (group + 1) * LANES]

    def final_copy(step):
        span = span_of(step)
        return pltpu.make_async_copy(final.at[span], final_ref.at[span], final_sem.at[0])

    def convolve(step):
        span = span_of(step)
        conv = []
        for group in range(groups):
            across = slice(group * LANES, (group + 1) * LANES)
            terms = [
                gated[group, pl.ds(step * tile + (PAD - taps // 2 + tap), tile), :] * depth[tap : tap + 1, across]
                for tap in range(taps)
            ]
            conv.append(functools.reduce(jnp.add, terms))
        conv = jnp.concatenate(conv, axis=1)
        activated = (conv * jax.nn.sigmoid(conv)).astype(bf16)
        after_conv = embedded[span, :] + dot_f32(activated, rest[3])
        final[span, :] = layer_norm(after_conv).astype(bf16)
        final_copy(step).start()

    ready = convolved = 0
    while convolved < tiles:
        if ready < tiles:
            count = 2 if ready + 4 <= tiles else 1
            gate(ready, count)
            if ready == 0:
                second[turn[-1]].finish()
            ready += count
        limit = tiles if ready == tiles else ready - 1
        while convolved < limit:
            convolve(convolved)
            convolved += 1

    for shift in range(1, levels):
        for kind in range(4):
            over_level(kind, shift).wait_send()

        sent = tables.at[level, pl.ds(0, codes // CORES)]
        for kind in range(2):
            pltpu.make_async_remote_copy(
                src_ref=sent, dst_ref=sent,
                send_sem=table_send.at[kind, shift], recv_sem=table_recv.at[kind, shift, 0],
                device_id={"level": level}, device_id_type=MESH,
            ).wait_send()
        sent = attended.at[:, own_columns]
        pltpu.make_async_remote_copy(
            src_ref=sent, dst_ref=sent,
            send_sem=att_send.at[shift], recv_sem=att_recv.at[0, shift],
            device_id={"level": level}, device_id_type=MESH,
        ).wait_send()

    pltpu.make_async_copy(final, final_ref, final_sem.at[0]).wait()


def decode_step(levels, devices, tokens, decoded, done, fill, table, w_qkv, w_out_t, w_expand, w_project, taps):
    frames, width = tokens.shape[1], table.shape[1]
    chips = devices // CORES
    columns = width // levels
    chunks = table.shape[0] // (CORES * LANES)
    tiles = frames // (2 * LANES)
    vmem = pl.BlockSpec(memory_space=pltpu.VMEM)
    anywhere = pl.BlockSpec(memory_space=pl.ANY)
    dma = pltpu.SemaphoreType.DMA
    half = chips // 2
    bf16, f32 = jnp.bfloat16, jnp.float32
    return pl.pallas_call(
        functools.partial(step_kernel, levels, devices, frames, width),
        out_shape=jax.ShapeDtypeStruct((frames, width), bf16),
        in_specs=[anywhere] * 2 + [pl.BlockSpec(memory_space=pltpu.SMEM)] + [anywhere] * 6 + [vmem],
        out_specs=anywhere,
        scratch_shapes=[
            pltpu.VMEM((levels,) + tokens.shape, jnp.int32),
            pltpu.VMEM((levels,) + decoded.shape, jnp.int32),
            pltpu.VMEM((levels,) + fill.shape, bf16),
            pltpu.VMEM((levels, frames, LANES), f32),
            pltpu.VMEM((levels,) + table.shape, bf16),
            pltpu.VMEM((3, width, columns), bf16),
            pltpu.VMEM((4, width, width), bf16),
            pltpu.VMEM((frames, width), f32),
            pltpu.VMEM((frames, columns), bf16),
            pltpu.VMEM((columns // (width // HEADS), width // HEADS + 16, frames), bf16),
            pltpu.VMEM((frames, columns), bf16),
            pltpu.VMEM((4 * LANES, width), bf16),
            pltpu.VMEM((4 * LANES, width), bf16),
            pltpu.VMEM((frames, width), bf16),
            pltpu.VMEM((width // LANES, frames + 2 * PAD, LANES), f32),
            pltpu.VMEM((frames, width), bf16),
            pltpu.VMEM((frames, 2 * LANES), f32),
            pltpu.VMEM((frames, 2 * LANES), f32),
            pltpu.VMEM((8, 2 * LANES), f32),
            pltpu.VMEM((8, 2 * LANES), f32),
            dma((11,)),
            dma((4, levels)), dma((4, levels)), dma((2, levels)), dma((2, levels, chunks)),
            dma((levels,)), dma((tiles + columns // LANES - 1, levels)), dma((1,)),
        ]
        + [
            dma(shape) for count in (3, 4) for shape in ((count,), (count, 2, half), (count,), (count,))
        ],
        compiler_params=pltpu.CompilerParams(
            collective_id=0, has_side_effects=True, vmem_limit_bytes=64000 * 1024
        ),
    )(tokens, decoded, done, fill, table, w_qkv, w_out_t, w_expand, w_project, taps)


def head_kernel(parts, final_ref, head_ref, logits_ref, final, head, logits, final_sem, head_sem, logits_sem):
    rows, columns = final.shape[0] // parts, head.shape[1] // 2
    spans = [pl.ds(part * rows, rows) for part in range(parts)]
    sides = [pl.ds(side * columns, columns) for side in range(2)]
    finals = [pltpu.make_async_copy(final_ref.at[span], final.at[span], final_sem.at[i]) for i, span in enumerate(spans)]
    heads = [pltpu.make_async_copy(head_ref.at[:, side], head.at[:, side], head_sem.at[i]) for i, side in enumerate(sides)]
    outs = [pltpu.make_async_copy(logits.at[span], logits_ref.at[span], logits_sem.at[i]) for i, span in enumerate(spans)]
    for copy in finals[:1] + heads + finals[1:]:
        copy.start()
    for part, span in enumerate(spans):
        finals[part].wait()
        for which, side in enumerate(sides):
            if part == 0:
                heads[which].wait()
            logits[span, side] = dot_f32(final[span, :], head[:, side]).astype(logits.dtype)
        outs[part].start()
    for copy in outs:
        copy.wait()


def score(final, head):
    frames, codes = final.shape[0], head.shape[1]
    parts = 3
    hbm = pl.BlockSpec(memory_space=pltpu.HBM)
    dma = pltpu.SemaphoreType.DMA
    return pl.pallas_call(
        functools.partial(head_kernel, parts),
        out_shape=jax.ShapeDtypeStruct((frames, codes), final.dtype),
        in_specs=[hbm, hbm],
        out_specs=hbm,
        scratch_shapes=[
            pltpu.VMEM(final.shape, final.dtype), pltpu.VMEM(head.shape, head.dtype),
            pltpu.VMEM((frames, codes), final.dtype), dma((parts,)), dma((2,)), dma((parts,)),
        ],
    )(final, head)


def body(
    token_ids,
    decoded_mask,
    levels_done,
    code_tables,
    mask_vectors,
    w_qkv,
    w_out,
    w_expand,
    w_depth,
    w_project,
    level_heads,
):
    final = decode_step(
        lax.axis_size("level"), lax.axis_size("dp"), token_ids[0], decoded_mask[0], levels_done, mask_vectors,
        code_tables[0], w_qkv, w_out.T, w_expand, w_project, w_depth,
    )
    return score(final, level_heads[0])[None, None]


def solution(mesh):
    return jax.shard_map(
        body,
        mesh=mesh,
        in_specs=(
            P("dp", "level", None),
            P("dp", "level", None),
            P("dp"),
            P("level", None, None),
            P("level", None),
            P(None, "dp", "level"),
            P("level", "dp"),
            P("dp", None),
            P(),
            P("dp", None),
            P("level", None, None),
        ),
        out_specs=P("dp", "level", None, None),
        check_vma=False,
    )
```
